8 devices in a mesh: stage: 4 (over z, y, x), data: 2 (over core).
Axes of the slice: x: 2, y: 2, z: 1, core: 2. Of those that a mesh axis runs over, the one named last changes fastest.
Arguments:
- inputs: bfloat16 [8, 1024, 2048], P('data')
- targets: bfloat16 [8, 1024, 2048], P('data')
- w_up: bfloat16 [4, 2048, 8192], P('stage')
- w_down: bfloat16 [4, 8192, 2048], P('stage')
Outputs:
- output 1: float32 [], replicated
- output 2: float32 [4, 2048, 8192], P('stage', 'data')
- output 3: float32 [4, 8192, 2048], P('stage', None, 'data')
All inputs are finite; a program needn't handle non-finite values.
Results may differ from the reference program's by a relative error of at most 0.00277113.
Values are sent between devices in bfloat16 or wider.
A program may use at most 1 GiB of HBM per device.

```python
import jax
import jax.numpy as jnp
from jax import lax

DATA_REPLICAS = 2
MICRO = 4
TOKENS = 1024
D_MODEL = 2048
FFN = 8192
LAYERS = 4


def setup_inputs(seed: int = 0) -> dict:
    root_key = jax.random.key(seed)
    key_inputs, key_targets, key_up, key_down = jax.random.split(root_key, 4)
    n_rows = DATA_REPLICAS * MICRO
    inputs = jax.random.normal(key_inputs, (n_rows, TOKENS, D_MODEL), jnp.float32)
    targets = jax.random.normal(key_targets, (n_rows, TOKENS, D_MODEL), jnp.float32)
    w_up = jax.random.normal(key_up, (LAYERS, D_MODEL, FFN), jnp.float32) * D_MODEL ** -0.5
    w_down = jax.random.normal(key_down, (LAYERS, FFN, D_MODEL), jnp.float32) * 1.5 * (FFN * LAYERS) ** -0.5
    return {'inputs': inputs.astype(jnp.bfloat16), 'targets': targets.astype(jnp.bfloat16), 'w_up': w_up.astype(jnp.bfloat16), 'w_down': w_down.astype(jnp.bfloat16)}


def layer_forward(h_in, w_up, w_down):
    pre_act = jnp.dot(h_in, w_up, preferred_element_type=jnp.float32)
    gelu_out = jax.nn.gelu(pre_act).astype(jnp.bfloat16)
    branch = jnp.dot(gelu_out, w_down, preferred_element_type=jnp.float32)
    return (h_in.astype(jnp.float32) + branch).astype(jnp.bfloat16)


def layer_backward(h_in, grad_out, w_up, w_down):
    pre_act = jnp.dot(h_in, w_up, preferred_element_type=jnp.float32)
    gelu_full, gelu_vjp = jax.vjp(jax.nn.gelu, pre_act)
    gelu_out = gelu_full.astype(jnp.bfloat16)
    g_down = jnp.dot(gelu_out.T, grad_out, preferred_element_type=jnp.float32)
    grad_act = jnp.dot(grad_out, w_down.T, preferred_element_type=jnp.float32).astype(jnp.bfloat16)
    grad_pre = gelu_vjp(grad_act.astype(jnp.float32))[0].astype(jnp.bfloat16)
    g_up = jnp.dot(h_in.T, grad_pre, preferred_element_type=jnp.float32)
    back_prod = jnp.dot(grad_pre, w_up.T, preferred_element_type=jnp.float32)
    grad_in = (grad_out.astype(jnp.float32) + back_prod).astype(jnp.bfloat16)
    return grad_in, g_up, g_down


def reference(inputs, targets, w_up, w_down):
    inv_total = 1.0 / (inputs.shape[0] * inputs.shape[1])

    def fwd_step(h_cur, weights):
        return layer_forward(h_cur, weights[0], weights[1]), h_cur

    def bwd_step(grad_cur, packed):
        grad_in, g_up, g_down = layer_backward(packed[0], grad_cur, packed[1], packed[2])
        return grad_in, (g_up, g_down)

    def one_micro(loop_state, mb_pair):
        acc_up, acc_down, loss_sum = loop_state
        h_last, layer_ins = lax.scan(fwd_step, mb_pair[0], (w_up, w_down))
        resid_diff = h_last.astype(jnp.float32) - mb_pair[1].astype(jnp.float32)
        top_grad = (resid_diff * inv_total).astype(jnp.bfloat16)
        scan_out = lax.scan(bwd_step, top_grad, (layer_ins, w_up, w_down), reverse=True)
        grads_up, grads_down = scan_out[1]
        new_state = (acc_up + grads_up, acc_down + grads_down, loss_sum + jnp.sum(resid_diff * resid_diff))
        return new_state, None

    init_state = (jnp.zeros(w_up.shape, jnp.float32), jnp.zeros(w_down.shape, jnp.float32), jnp.zeros((), jnp.float32))
    final_state = lax.scan(one_micro, init_state, (inputs, targets))[0]
    return final_state[2] * (0.5 * inv_total), final_state[0], final_state[1]
```

```python
import jax
import jax.numpy as jnp
from jax import lax
from jax.sharding import PartitionSpec as P

CONTRACT_ROWS = (((0,), (0,)), ((), ()))
CONTRACT_COLS = (((1,), (1,)), ((), ()))
C0 = 0.7978845608028654
C1 = 0.044715
CHUNK = 512


def gelu_and_slope(u):
    u2 = u * u
    half = 0.5 * jnp.tanh(u * (C0 + (C0 * C1) * u2)) + 0.5
    g = u * half
    slope = half + (g * (1.0 - half)) * (2.0 * C0 + (6.0 * C0 * C1) * u2)
    return g.astype(jnp.bfloat16), slope


def solution(mesh):
    n_stage = mesh.shape['stage']
    n_data = mesh.shape['data']
    fwd_perm = [(k, k + 1) for k in range(n_stage - 1)]
    bwd_perm = [(k + 1, k) for k in range(n_stage - 1)]

    def per_device(inputs, targets, w_up, w_down):
        n_micro, n_tok, width = inputs.shape
        ffn = w_up.shape[2]
        rows = n_micro * n_tok
        n_chunk = rows // CHUNK
        x = inputs.reshape(rows, width)
        y = targets.reshape(rows, width)
        w1 = w_up[0]
        w2 = w_down[0]
        stage_id = lax.axis_index('stage')
        is_first = stage_id == 0
        is_last = stage_id == n_stage - 1
        inv_total = 1.0 / (n_data * rows)
        spare = rows

        def rows_of(a, at):
            return lax.dynamic_slice_in_dim(a, at, CHUNK, 0)

        def put(a, v, at):
            return lax.dynamic_update_slice_in_dim(a, v, at, 0)

        def tick(t, st):
            recv_f, recv_b, sh, sg, sd, sq, se, loss = st
            f = t - stage_id
            f_ok = (f >= 0) & (f < n_chunk)
            f_at = jnp.clip(f, 0, n_chunk - 1) * CHUNK
            f_to = jnp.where(f_ok, f_at, spare)
            h = jnp.where(is_first, rows_of(x, f_at), recv_f)
            g, d = gelu_and_slope(jnp.dot(h, w1, preferred_element_type=jnp.float32))
            sg = put(sg, g, f_to)
            sd = put(sd, d, f_to)
            sh = put(sh, h, f_to)
            v = jnp.dot(g, w2, preferred_element_type=jnp.float32)
            h_out = (h.astype(jnp.float32) + v).astype(jnp.bfloat16)
            send_f = lax.ppermute(h_out, 'stage', fwd_perm)
            diff = h_out.astype(jnp.float32) - rows_of(y, f_at).astype(jnp.float32)
            loss = loss + jnp.where(f_ok & is_last, jnp.sum(diff * diff), 0.0)
            top = (diff * inv_total).astype(jnp.bfloat16)

            b = t - (2 * (n_stage - 1) - stage_id)
            b_ok = (b >= 0) & (b < n_chunk)
            b_at = jnp.clip(b, 0, n_chunk - 1) * CHUNK
            b_to = jnp.where(b_ok, b_at, spare)
            e = jnp.where(is_last, top, recv_b)
            p = lax.dot_general(e, w2, CONTRACT_COLS, preferred_element_type=jnp.float32).astype(jnp.bfloat16)
            q = (p.astype(jnp.float32) * rows_of(sd, b_at)).astype(jnp.bfloat16)
            sq = put(sq, q, b_to)
            se = put(se, e, b_to)
            back = lax.dot_general(q, w1, CONTRACT_COLS, preferred_element_type=jnp.float32)
            e_out = (e.astype(jnp.float32) + back).astype(jnp.bfloat16)
            send_b = lax.ppermute(e_out, 'stage', bwd_perm)
            return send_f, send_b, sh, sg, sd, sq, se, loss

        def zeros(cols, dt=jnp.bfloat16):
            return jnp.zeros((rows + CHUNK, cols), dt)

        z = jnp.zeros((CHUNK, width), jnp.bfloat16)
        init = (z, z, zeros(width), zeros(ffn), zeros(ffn, jnp.float32), zeros(ffn), zeros(width), jnp.zeros((), jnp.float32))
        n_tick = n_chunk + 2 * (n_stage - 1)
        _, _, sh, sg, _, sq, se, loss = lax.fori_loop(0, n_tick, tick, init)
        half = width // n_data
        mine = lax.axis_index('data') * half
        other = (n_data - 1) * half - mine
        swap = [(0, 1), (1, 0)]
        sh, sg, sq, se = sh[:rows], sg[:rows], sq[:rows], se[:rows]

        def cols(a, at):
            return lax.dynamic_slice_in_dim(a, at, half, 1)

        def tn(a, b):
            return lax.dot_general(a, b, CONTRACT_ROWS, preferred_element_type=jnp.float32)

        up_other = lax.ppermute(tn(cols(sh, other), sq), 'data', swap)
        down_other = lax.ppermute(tn(sg, cols(se, other)), 'data', swap)
        g_up = tn(cols(sh, mine), sq) + up_other
        g_down = tn(sg, cols(se, mine)) + down_other
        loss_total = lax.psum(loss, ('stage', 'data')) * (0.5 * inv_total)
        return loss_total, g_up[None], g_down[None]

    return jax.shard_map(per_device, mesh=mesh, in_specs=(P('data', None, None), P('data', None, None), P('stage', None, None), P('stage', None, None)), out_specs=(P(), P('stage', 'data', None), P('stage', None, 'data')), check_vma=False)
```

```python
import functools

import jax
import jax.numpy as jnp
from jax import lax
from jax.experimental import pallas as pl
from jax.experimental.pallas import tpu as pltpu
from jax.sharding import PartitionSpec as P

BF16 = jnp.bfloat16
F32 = jnp.float32
C0 = 0.7978845608028654
C1 = 0.044715
ROWS = 256
CT = 1024
DT = 512
NSTEP = 4
RING = 4
NN = (((1,), (0,)), ((), ()))
NT = (((1,), (1,)), ((), ()))
TN = (((0,), (0,)), ((), ()))


def dot(a, b, dims):
    return lax.dot_general(a, b, dims, preferred_element_type=F32)


def pipeline_kernel(n_stage, n_data, n_chunk, inv_total,
                    x, y, w1, w2,
                    hs, gs, ds, qs, es, loss_out,
                    w1r, w2r, ring, gq, dbuf, inb, out, loss_acc, lbuf,
                    w1_sem, w2_sem, ring_sem, d_sem, gq_sem, in_sem, o_send,
                    h_recv, e_recv, y_sem, st_sem, l_send, l_recv):
    s = lax.axis_index('stage')
    peer = n_data - 1 - lax.axis_index('data')
    first = s == 0
    last = s == n_stage - 1
    half = w1r.shape[1]
    n_slot = 2 * n_chunk
    warm = n_chunk - 5 * s

    def order(k):
        j = jnp.maximum(k - warm, 0)
        left = n_chunk - warm
        early = k < warm
        mixed = j < 2 * left
        odd = lax.rem(j, 2) == 1
        is_f = early | (mixed & odd)
        idx = jnp.where(early, k, jnp.where(mixed, jnp.where(odd, warm + j // 2, j // 2), j - left))
        return is_f, idx

    def rows(i):
        return pl.ds(pl.multiple_of(i * ROWS, ROWS), ROWS)

    def cols(j, size, base=0):
        if isinstance(j, int):
            return pl.ds(base + j * size, size)
        return pl.ds(pl.multiple_of(base + j * size, size), size)

    def copy(src, dst, sem):
        return pltpu.make_async_copy(src, dst, sem)

    def start_f1(j):
        copy(w1.at[0, :, cols(j, CT, half)], ring.at[j], ring_sem.at[j]).start()

    def start_f2(j):
        for i in range(2):
            copy(w2.at[0, pl.ds(half + i * 2048, 2048), cols(j, DT)], ring.at[j, :, pl.ds(i * DT, DT)], ring_sem.at[j]).start()

    def start_b1(j):
        for i in range(2):
            copy(w2.at[0, cols(j, CT, half), pl.ds(i * CT, CT)], ring.at[j, pl.ds(i * CT, CT)], ring_sem.at[j]).start()

    def start_b2(j):
        for i in range(4):
            copy(w1.at[0, cols(j, DT), pl.ds(half + i * CT, CT)], ring.at[j, pl.ds(i * DT, DT)], ring_sem.at[j]).start()

    def start_slot(k, j):
        is_f, _ = order(k)

        @pl.when((k < n_slot) & is_f)
        def _():
            start_f1(j)

        @pl.when((k < n_slot) & jnp.logical_not(is_f))
        def _():
            start_b1(j)

    def wait_ring(r):
        copy(ring.at[r], ring.at[r], ring_sem.at[r]).wait()

    def d_cols(j, b):
        return cols(j, CT, b * half)

    def d_out_slot(j, b):
        return 2 + lax.rem(j, 3) if b else lax.rem(j, 2)

    def d_in_slot(j, b):
        return 3 * b + lax.rem(j, 2)

    def start_d_in(i, j):
        for b in range(2):
            copy(ds.at[rows(i), d_cols(j, b)], dbuf.at[d_in_slot(j, b)], d_sem.at[d_in_slot(j, b)]).start()

    def start_d_out(i, j, b):
        copy(dbuf.at[d_out_slot(j, b)], ds.at[rows(i), d_cols(j, b)], d_sem.at[d_out_slot(j, b)]).start()

    def wait_d(q):
        copy(dbuf.at[q], dbuf.at[q], d_sem.at[q]).wait()

    def needs_copy(k):
        is_f, _ = order(k)
        return is_f | jnp.logical_not(last)

    def ahead(k):
        return (first | (k >= warm)) & (k < n_slot)

    def load_in(k):
        is_f, i = order(k)
        b = lax.rem(k, 2)

        @pl.when(is_f & first)
        def _():
            copy(x.at[rows(i)], inb.at[b], in_sem.at[b]).start()

        @pl.when(is_f & jnp.logical_not(first))
        def _():
            copy(hs.at[rows(i)], hs.at[rows(i)], h_recv.at[i]).wait()
            copy(hs.at[rows(i)], inb.at[b], in_sem.at[b]).start()

        @pl.when(jnp.logical_not(is_f) & jnp.logical_not(last))
        def _():
            copy(es.at[rows(i)], es.at[rows(i)], e_recv.at[i]).wait()
            copy(es.at[rows(i)], inb.at[b], in_sem.at[b]).start()

    def before_next(k):
        is_f, i = order(k + 1)

        @pl.when(ahead(k + 1))
        def _():
            load_in(k + 1)

        @pl.when((k + 1 < n_slot) & jnp.logical_not(is_f))
        def _():
            start_d_in(i, 0)

    def next_stage(k, i, j):
        o = lax.rem(k, 2)
        return pltpu.make_async_remote_copy(
            src_ref=out.at[o, :, cols(j, DT)], dst_ref=hs.at[rows(i), cols(j, DT)],
            send_sem=o_send.at[o], recv_sem=h_recv.at[i],
            device_id={'stage': s + 1}, device_id_type=pl.DeviceIdType.MESH)

    def prev_stage(k, i, j):
        o = lax.rem(k, 2)
        return pltpu.make_async_remote_copy(
            src_ref=out.at[o, :, cols(j, DT)], dst_ref=es.at[rows(i), cols(j, DT)],
            send_sem=o_send.at[o], recv_sem=e_recv.at[i],
            device_id={'stage': s - 1}, device_id_type=pl.DeviceIdType.MESH)

    def sent(k):
        is_f, _ = order(k)
        return (is_f & jnp.logical_not(last)) | (jnp.logical_not(is_f) & jnp.logical_not(first))

    def wait_sent(k):
        @pl.when((k >= 0) & sent(jnp.maximum(k, 0)))
        def _():
            o = lax.rem(k, 2)
            copy(out.at[o], out.at[o], o_send.at[o]).wait()

    def gelu_tile(q, c):
        for r in range(0, ROWS, 16):
            for z in range(0, CT, 256):
                u = dbuf[q, pl.ds(r, 16), pl.ds(z, 256)]
                u2 = u * u
                h = 0.5 * jnp.tanh(u * (C0 + (C0 * C1) * u2)) + 0.5
                g = u * h
                gq[pl.ds(r, 16), pl.ds(pl.multiple_of(c + z, 256), 256)] = g.astype(BF16)
                dbuf[q, pl.ds(r, 16), pl.ds(z, 256)] = h + (g * (1.0 - h)) * (2.0 * C0 + (6.0 * C0 * C1) * u2)

    def g_out(i, j, b):
        copy(gq.at[:, d_cols(j, b)], gs.at[rows(i), d_cols(j, b)], gq_sem).start()

    def forward(k, i):
        p = lax.rem(k, 2)
        o = lax.rem(k, 2)

        def step1(j, carry):
            @pl.when(j == 0)
            def _():
                start_f1(2)
                start_f1(3)

            @pl.when(j >= 1)
            def _():
                start_f2(j - 1)

            @pl.when(j >= 2)
            def _():
                wait_d(lax.rem(j, 2))

            @pl.when(j >= 3)
            def _():
                wait_d(2)

            @pl.when(k == 0)
            def _():
                copy(w1r.at[:, cols(j, CT)], w1r.at[:, cols(j, CT)], w1_sem.at[j]).wait()

            wait_ring(j)
            jp = jnp.maximum(j - 1, 0)
            dbuf[d_out_slot(j, 0)] = dot(inb[p], w1r[:, cols(j, CT)], NN)
            gelu_tile(2 + lax.rem(j + 2, 3), half + jp * CT)
            dbuf[d_out_slot(j, 1)] = dot(inb[p], ring[j], NN)
            gelu_tile(d_out_slot(j, 0), j * CT)

            @pl.when(j >= 1)
            def _():
                g_out(i, j - 1, 1)
                start_d_out(i, j - 1, 1)

            g_out(i, j, 0)
            start_d_out(i, j, 0)
            return carry

        lax.fori_loop(0, NSTEP, step1, 0)

        @pl.when(last)
        def _():
            copy(inb.at[1 - p], inb.at[1 - p], y_sem).wait()

        wait_sent(k - 2)
        for jj in range(2):
            if jj == 0:
                start_f2(3)
                wait_d(3)
            else:
                start_slot(k + 1, 0)
                start_slot(k + 1, 1)
                for q in (0, 1, 4):
                    wait_d(q)
                before_next(k)

            @pl.when(k == 0)
            def _():
                for j in (2 * jj, 2 * jj + 1):
                    copy(w2r.at[:, cols(j, DT)], w2r.at[:, cols(j, DT)], w2_sem.at[j]).wait()

            for j in (2 * jj, 2 * jj + 1):
                wait_ring(j)
            for j in (2 * jj, 2 * jj + 1):
                v = dot(gq[:, pl.ds(0, half)], w2r[:, cols(j, DT)], NN)
                if j == 0:
                    dbuf[3, :, pl.ds(0, DT)] = v
                    gelu_tile(2, half + 3 * CT)
                    v = dbuf[3, :, pl.ds(0, DT)]
                v = v + dot(gq[:, pl.ds(half, 2048)], ring[j, :, pl.ds(0, DT)], NN)
                v = v + dot(gq[:, pl.ds(half + 2048, 2048)], ring[j, :, pl.ds(DT, DT)], NN)
                out[o, :, cols(j, DT)] = (inb[p, :, cols(j, DT)].astype(F32) + v).astype(BF16)
            if jj == 0:
                g_out(i, 3, 1)
                start_d_out(i, 3, 1)

            @pl.when(jnp.logical_not(last))
            def _():
                for j in (2 * jj, 2 * jj + 1):
                    next_stage(k, i, j).start()

            @pl.when(last)
            def _():
                for j in (2 * jj, 2 * jj + 1):
                    for r in range(0, ROWS, 16):
                        diff = out[o, pl.ds(r, 16), cols(j, DT)].astype(F32) - inb[1 - p, pl.ds(r, 16), cols(j, DT)].astype(F32)
                        loss_acc[...] += diff * diff
                        inb[1 - p, pl.ds(r, 16), cols(j, DT)] = (diff * inv_total).astype(BF16)

        wait_d(2)

    def backward(k, i):
        p = lax.rem(k, 2)
        o = lax.rem(k, 2)

        def step1(j, carry):
            @pl.when(j == 0)
            def _():
                start_b1(2)
                start_b1(3)

            @pl.when((j >= 1) & jnp.logical_not(first))
            def _():
                start_b2(j - 1)

            @pl.when((j >= 1) & (j < 3) & first)
            def _():
                start_slot(k + 1, j - 1)

            @pl.when(j < NSTEP - 1)
            def _():
                start_d_in(i, j + 1)

            @pl.when((j == NSTEP - 1) & first)
            def _():
                before_next(k)

            wait_d(d_in_slot(j, 0))
            wait_d(d_in_slot(j, 1))
            wait_ring(j)
            pa = dot(inb[p], w2r[cols(j, CT), :], NT).astype(BF16).astype(F32)
            gq[:, d_cols(j, 0)] = (pa * dbuf[d_in_slot(j, 0)]).astype(BF16)
            pb = dot(inb[p, :, pl.ds(0, CT)], ring[j, pl.ds(0, CT)], NT)
            pb = pb + dot(inb[p, :, pl.ds(CT, CT)], ring[j, pl.ds(CT, CT)], NT)
            pb = pb.astype(BF16).astype(F32)
            gq[:, d_cols(j, 1)] = (pb * dbuf[d_in_slot(j, 1)]).astype(BF16)
            for b in range(2):
                copy(gq.at[:, d_cols(j, b)], qs.at[rows(i), d_cols(j, b)], gq_sem).start()
            return carry

        lax.fori_loop(0, NSTEP, step1, 0)
        wait_sent(k - 2)

        @pl.when(jnp.logical_not(first))
        def _():
            def step2(jj, carry):
                @pl.when(jj == 0)
                def _():
                    start_b2(3)

                @pl.when(jj == 1)
                def _():
                    start_slot(k + 1, 0)
                    start_slot(k + 1, 1)
                    before_next(k)

                for z in range(2):
                    wait_ring(2 * jj + z)
                for z in range(2):
                    j = 2 * jj + z
                    v = dot(gq[:, pl.ds(0, half)], w1r[cols(j, DT), :], NT)
                    for c in range(4):
                        v = v + dot(gq[:, pl.ds(half + c * CT, CT)], ring[j, pl.ds(c * DT, DT)], NT)
                    out[o, :, cols(j, DT)] = (inb[p, :, cols(j, DT)].astype(F32) + v).astype(BF16)
                for z in range(2):
                    prev_stage(k, i, 2 * jj + z).start()
                return carry

            lax.fori_loop(0, 2, step2, 0)

    barrier = pltpu.get_barrier_semaphore()

    def hello(**to):
        pl.semaphore_signal(barrier, inc=1, device_id=to, device_id_type=pl.DeviceIdType.MESH)

    @pl.when(jnp.logical_not(first))
    def _():
        hello(stage=s - 1)

    @pl.when(jnp.logical_not(last))
    def _():
        hello(stage=s + 1)

    @pl.when(last)
    def _():
        hello(data=peer)

    @pl.when(first)
    def _():
        load_in(0)

    start_f1(0)
    for j in range(NSTEP):
        copy(w1.at[0, :, pl.ds(j * CT, CT)], w1r.at[:, pl.ds(j * CT, CT)], w1_sem.at[j]).start()
        if j == 0:
            start_f1(1)
    for j in range(NSTEP):
        copy(w2.at[0, pl.ds(0, half), pl.ds(j * DT, DT)], w2r.at[:, pl.ds(j * DT, DT)], w2_sem.at[j]).start()
    loss_acc[...] = jnp.zeros_like(loss_acc)

    @pl.when(first)
    def _():
        pl.semaphore_wait(barrier, 1)

    @pl.when(jnp.logical_not(first))
    def _():
        pl.semaphore_wait(barrier, 2)

    def slot(k, carry):
        is_f, i = order(k)
        p = lax.rem(k, 2)

        @pl.when(k > 0)
        def _():
            copy(gq, gq, gq_sem).wait()

        @pl.when(jnp.logical_not(ahead(k)))
        def _():
            load_in(k)

        @pl.when(needs_copy(k))
        def _():
            copy(inb.at[p], inb.at[p], in_sem.at[p]).wait()

        @pl.when(is_f & first)
        def _():
            copy(inb.at[p], hs.at[rows(i)], st_sem).start()

        @pl.when(jnp.logical_not(is_f) & last)
        def _():
            copy(inb.at[p], es.at[rows(i)], st_sem).start()

        @pl.when(is_f & last)
        def _():
            copy(y.at[rows(i)], inb.at[1 - p], y_sem).start()

        @pl.when(is_f)
        def _():
            forward(k, i)

        @pl.when(jnp.logical_not(is_f))
        def _():
            backward(k, i)

        @pl.when((is_f & first) | (jnp.logical_not(is_f) & last))
        def _():
            copy(inb.at[p], inb.at[p], st_sem).wait()

        return carry

    lax.fori_loop(0, n_slot, slot, 0)
    copy(gq, gq, gq_sem).wait()
    for k in range(n_slot - 2, n_slot):
        wait_sent(jnp.int32(k))

    def to_peer():
        return pltpu.make_async_remote_copy(
            src_ref=lbuf.at[0], dst_ref=lbuf.at[1], send_sem=l_send.at[0], recv_sem=l_recv.at[0],
            device_id={'data': peer}, device_id_type=pl.DeviceIdType.MESH)

    def to_prev():
        return pltpu.make_async_remote_copy(
            src_ref=lbuf.at[2], dst_ref=lbuf.at[2], send_sem=l_send.at[1], recv_sem=l_recv.at[1],
            device_id={'stage': s - 1}, device_id_type=pl.DeviceIdType.MESH)

    @pl.when(last)
    def _():
        lbuf[0] = loss_acc[pl.ds(0, 8), :] + loss_acc[pl.ds(8, 8), :]
        rdma = to_peer()
        rdma.start()
        rdma.wait()
        lbuf[2] = lbuf[0] + lbuf[1]

    @pl.when(jnp.logical_not(last))
    def _():
        copy(lbuf.at[2], lbuf.at[2], l_recv.at[1]).wait()

    loss_out[...] = lbuf[2]

    @pl.when(jnp.logical_not(first))
    def _():
        to_prev().start()
        copy(lbuf.at[2], lbuf.at[2], l_send.at[1]).wait()


def run_pipeline(n_stage, n_data, x, y, w1, w2):
    n_row, width = x.shape
    ffn = w1.shape[2]
    n_chunk = n_row // ROWS
    half = ffn // 2
    hbm = pl.BlockSpec(memory_space=pl.ANY)
    out = jax.ShapeDtypeStruct
    dma = pltpu.SemaphoreType.DMA
    flops = 8 * n_row * width * ffn
    return pl.pallas_call(
        functools.partial(pipeline_kernel, n_stage, n_data, n_chunk, 1.0 / (n_data * n_row)),
        out_shape=(out((n_row, width), BF16), out((n_row, ffn), BF16), out((n_row, ffn), F32),
                   out((n_row, ffn), BF16), out((n_row, width), BF16), out((8, DT), F32)),
        in_specs=[hbm] * 4,
        out_specs=(hbm,) * 5 + (pl.BlockSpec(memory_space=pltpu.VMEM),),
        scratch_shapes=[
            pltpu.VMEM((width, half), BF16), pltpu.VMEM((half, width), BF16),
            pltpu.VMEM((RING, width, CT), BF16), pltpu.VMEM((ROWS, ffn), BF16),
            pltpu.VMEM((5, ROWS, CT), F32), pltpu.VMEM((2, ROWS, width), BF16),
            pltpu.VMEM((2, ROWS, width), BF16), pltpu.VMEM((16, DT), F32),
            pltpu.VMEM((3, 8, DT), F32),
            dma((NSTEP,)), dma((NSTEP,)), dma((RING,)), dma((5,)), dma, dma((2,)), dma((2,)),
            dma((n_chunk,)), dma((n_chunk,)), dma, dma, dma((2,)), dma((2,)),
        ],
        compiler_params=pltpu.CompilerParams(collective_id=0, has_side_effects=True, vmem_limit_bytes=67043328),
        cost_estimate=pl.CostEstimate(flops=flops, bytes_accessed=1 << 30, transcendentals=n_row * ffn),
        name='pipeline',
    )(x, y, w1, w2)


def solution(mesh):
    n_stage = mesh.shape['stage']
    n_data = mesh.shape['data']

    def per_device(inputs, targets, w_up, w_down):
        n_micro, n_tok, width = inputs.shape
        n_row = n_micro * n_tok
        x = inputs.reshape(n_row, width)
        y = targets.reshape(n_row, width)
        hs, gs, _, qs, es, loss = run_pipeline(n_stage, n_data, x, y, w_up, w_down)
        half = width // n_data
        mine = lax.axis_index('data') * half
        other = (n_data - 1) * half - mine
        swap = [(0, 1), (1, 0)]

        def part(a, at):
            return lax.dynamic_slice_in_dim(a, at, half, 1)

        up_other = lax.ppermute(dot(part(hs, other), qs, TN), 'data', swap)
        down_other = lax.ppermute(dot(gs, part(es, other), TN), 'data', swap)
        g_up = dot(part(hs, mine), qs, TN) + up_other
        g_down = dot(gs, part(es, mine), TN) + down_other
        loss_total = jnp.sum(loss) * (0.5 / (n_data * n_row))
        return loss_total, g_up[None], g_down[None]

    return jax.shard_map(per_device, mesh=mesh, in_specs=(P('data', None, None), P('data', None, None), P('stage', None, None), P('stage', None, None)), out_specs=(P(), P('stage', 'data', None), P('stage', None, 'data')), check_vma=False)
```

```python
import functools

import jax
import jax.numpy as jnp
from jax import lax
from jax.experimental import pallas as pl
from jax.experimental.pallas import tpu as pltpu
from jax.sharding import PartitionSpec as P

BF16 = jnp.bfloat16
F32 = jnp.float32
C0 = 0.7978845608028654
C1 = 0.044715
ROWS = 256
CT = 1024
DT = 512
NSTEP = 4
RING = 4
NN = (((1,), (0,)), ((), ()))
NT = (((1,), (1,)), ((), ()))
TN = (((0,), (0,)), ((), ()))


def dot(a, b, dims):
    return lax.dot_general(a, b, dims, preferred_element_type=F32)


N_BLOCK = 16


def early_plan(s):
    n_unit = jnp.where(s == 0, 44, jnp.where(s == 1, 34, jnp.where(s == 2, 16, 0)))
    after = jnp.where(s == 2, 10, 8)
    each = jnp.where(s == 0, 44, jnp.where(s == 1, 5, 4))
    return n_unit, after, each


def pipeline_kernel(n_stage, n_data, n_chunk, inv_total,
                    x, y, w1, w2,
                    hs, gs, ds, qs, es, up_part, down_part, loss_out,
                    w1r, w2r, ring, gq, dbuf, inb, out, loss_acc, lbuf,
                    w1_sem, w2_sem, ring_sem, d_sem, gq_sem, in_sem, o_send,
                    h_recv, e_recv, y_sem, st_sem, l_send, l_recv, held_sem, tile_sem, part_sem):
    s = lax.axis_index('stage')
    peer = n_data - 1 - lax.axis_index('data')
    first = s == 0
    last = s == n_stage - 1
    half = w1r.shape[1]
    n_slot = 2 * n_chunk
    warm = n_chunk - 5 * s

    def order(k):
        j = jnp.maximum(k - warm, 0)
        left = n_chunk - warm
        early = k < warm
        mixed = j < 2 * left
        odd = lax.rem(j, 2) == 1
        is_f = early | (mixed & odd)
        idx = jnp.where(early, k, jnp.where(mixed, jnp.where(odd, warm + j // 2, j // 2), j - left))
        return is_f, idx

    def rows(i):
        return pl.ds(pl.multiple_of(i * ROWS, ROWS), ROWS)

    def cols(j, size, base=0):
        if isinstance(j, int):
            return pl.ds(base + j * size, size)
        return pl.ds(pl.multiple_of(base + j * size, size), size)

    def copy(src, dst, sem):
        return pltpu.make_async_copy(src, dst, sem)

    def start_f1(j):
        copy(w1.at[0, :, cols(j, CT, half)], ring.at[j], ring_sem.at[j]).start()

    def start_f2(j):
        for i in range(2):
            copy(w2.at[0, pl.ds(half + i * 2048, 2048), cols(j, DT)], ring.at[j, :, pl.ds(i * DT, DT)], ring_sem.at[j]).start()

    def start_b1(j):
        for i in range(2):
            copy(w2.at[0, cols(j, CT, half), pl.ds(i * CT, CT)], ring.at[j, pl.ds(i * CT, CT)], ring_sem.at[j]).start()

    def start_b2(j):
        for i in range(4):
            copy(w1.at[0, cols(j, DT), pl.ds(half + i * CT, CT)], ring.at[j, pl.ds(i * DT, DT)], ring_sem.at[j]).start()

    def start_slot(k, j):
        is_f, _ = order(k)

        @pl.when((k < n_slot) & is_f)
        def _():
            start_f1(j)

        @pl.when((k < n_slot) & jnp.logical_not(is_f))
        def _():
            start_b1(j)

    def wait_ring(r):
        copy(ring.at[r], ring.at[r], ring_sem.at[r]).wait()

    def d_cols(j, b):
        return cols(j, CT, b * half)

    def d_out_slot(j, b):
        return 2 + lax.rem(j, 3) if b else lax.rem(j, 2)

    def d_in_slot(j, b):
        return 3 * b + lax.rem(j, 2)

    def start_d_in(i, j):
        for b in range(2):
            copy(ds.at[rows(i), d_cols(j, b)], dbuf.at[d_in_slot(j, b)], d_sem.at[d_in_slot(j, b)]).start()

    def start_d_out(i, j, b):
        copy(dbuf.at[d_out_slot(j, b)], ds.at[rows(i), d_cols(j, b)], d_sem.at[d_out_slot(j, b)]).start()

    def wait_d(q):
        copy(dbuf.at[q], dbuf.at[q], d_sem.at[q]).wait()

    def needs_copy(k):
        is_f, _ = order(k)
        return is_f | jnp.logical_not(last)

    def ahead(k):
        return (first | (k >= warm)) & (k < n_slot)

    def load_in(k):
        is_f, i = order(k)
        b = lax.rem(k, 2)

        @pl.when(is_f & first)
        def _():
            copy(x.at[rows(i)], inb.at[b], in_sem.at[b]).start()

        @pl.when(is_f & jnp.logical_not(first))
        def _():
            copy(hs.at[rows(i)], hs.at[rows(i)], h_recv.at[i]).wait()
            copy(hs.at[rows(i)], inb.at[b], in_sem.at[b]).start()

        @pl.when(jnp.logical_not(is_f) & jnp.logical_not(last))
        def _():
            copy(es.at[rows(i)], es.at[rows(i)], e_recv.at[i]).wait()
            copy(es.at[rows(i)], inb.at[b], in_sem.at[b]).start()

    def before_next(k):
        is_f, i = order(k + 1)

        @pl.when(ahead(k + 1))
        def _():
            load_in(k + 1)

        @pl.when((k + 1 < n_slot) & jnp.logical_not(is_f))
        def _():
            start_d_in(i, 0)

    def next_stage(k, i, j):
        o = lax.rem(k, 2)
        return pltpu.make_async_remote_copy(
            src_ref=out.at[o, :, cols(j, DT)], dst_ref=hs.at[rows(i), cols(j, DT)],
            send_sem=o_send.at[o], recv_sem=h_recv.at[i],
            device_id={'stage': s + 1}, device_id_type=pl.DeviceIdType.MESH)

    def prev_stage(k, i, j):
        o = lax.rem(k, 2)
        return pltpu.make_async_remote_copy(
            src_ref=out.at[o, :, cols(j, DT)], dst_ref=es.at[rows(i), cols(j, DT)],
            send_sem=o_send.at[o], recv_sem=e_recv.at[i],
            device_id={'stage': s - 1}, device_id_type=pl.DeviceIdType.MESH)

    def sent(k):
        is_f, _ = order(k)
        return (is_f & jnp.logical_not(last)) | (jnp.logical_not(is_f) & jnp.logical_not(first))

    def wait_sent(k):
        @pl.when((k >= 0) & sent(jnp.maximum(k, 0)))
        def _():
            o = lax.rem(k, 2)
            copy(out.at[o], out.at[o], o_send.at[o]).wait()

    def gelu_tile(q, c, lo, hi):
        for r in range(0, ROWS, 16):
            for z in range(lo, hi, 256):
                u = dbuf[q, pl.ds(r, 16), pl.ds(z, 256)]
                u2 = u * u
                h = 0.5 * jnp.tanh(u * (C0 + (C0 * C1) * u2)) + 0.5
                g = u * h
                gq[pl.ds(r, 16), pl.ds(pl.multiple_of(c + z, 256), 256)] = g.astype(BF16)
                dbuf[q, pl.ds(r, 16), pl.ds(z, 256)] = h + (g * (1.0 - h)) * (2.0 * C0 + (6.0 * C0 * C1) * u2)

    def g_out(i, j, b):
        copy(gq.at[:, d_cols(j, b)], gs.at[rows(i), d_cols(j, b)], gq_sem).start()

    def forward(k, i):
        p = lax.rem(k, 2)
        o = lax.rem(k, 2)

        def step1(j, carry):
            @pl.when(j == 0)
            def _():
                start_f1(2)
                start_f1(3)

            @pl.when(j >= 1)
            def _():
                start_f2(j - 1)

            @pl.when(j >= 2)
            def _():
                wait_d(lax.rem(j, 2))

            @pl.when(j >= 3)
            def _():
                wait_d(2)

            @pl.when(k == 0)
            def _():
                copy(w1r.at[:, cols(j, CT)], w1r.at[:, cols(j, CT)], w1_sem.at[j]).wait()

            wait_ring(j)
            jp = jnp.maximum(j - 1, 0)
            res, stm, old = d_out_slot(j, 0), d_out_slot(j, 1), 2 + lax.rem(j + 2, 3)
            old_at, res_at = half + jp * CT, j * CT
            dbuf[res, :, pl.ds(0, DT)] = dot(inb[p], w1r[:, cols(2 * j, DT)], NN)
            gelu_tile(old, old_at, 0, 768)
            dbuf[res, :, pl.ds(DT, DT)] = dot(inb[p], w1r[:, cols(2 * j + 1, DT)], NN)
            gelu_tile(old, old_at, 768, CT)
            gelu_tile(res, res_at, 0, 512)
            dbuf[stm, :, pl.ds(0, DT)] = dot(inb[p], ring[j, :, pl.ds(0, DT)], NN)
            gelu_tile(res, res_at, 512, CT)
            dbuf[stm, :, pl.ds(DT, DT)] = dot(inb[p], ring[j, :, pl.ds(DT, DT)], NN)

            @pl.when(j >= 1)
            def _():
                g_out(i, j - 1, 1)
                start_d_out(i, j - 1, 1)

            g_out(i, j, 0)
            start_d_out(i, j, 0)
            return carry

        lax.fori_loop(0, NSTEP, step1, 0)

        @pl.when(last)
        def _():
            copy(inb.at[1 - p], inb.at[1 - p], y_sem).wait()

        wait_sent(k - 2)
        for jj in range(2):
            if jj == 0:
                start_f2(3)
                wait_d(3)
            else:
                start_slot(k + 1, 0)
                start_slot(k + 1, 1)
                for q in (0, 1, 4):
                    wait_d(q)
                before_next(k)

            @pl.when(k == 0)
            def _():
                for j in (2 * jj, 2 * jj + 1):
                    copy(w2r.at[:, cols(j, DT)], w2r.at[:, cols(j, DT)], w2_sem.at[j]).wait()

            for j in (2 * jj, 2 * jj + 1):
                wait_ring(j)
            for j in (2 * jj, 2 * jj + 1):
                v = dot(gq[:, pl.ds(0, half)], w2r[:, cols(j, DT)], NN)
                if j == 0:
                    dbuf[3, :, pl.ds(0, DT)] = v
                    gelu_tile(2, half + 3 * CT, 0, CT)
                    v = dbuf[3, :, pl.ds(0, DT)]
                v = v + dot(gq[:, pl.ds(half, 2048)], ring[j, :, pl.ds(0, DT)], NN)
                v = v + dot(gq[:, pl.ds(half + 2048, 2048)], ring[j, :, pl.ds(DT, DT)], NN)
                out[o, :, cols(j, DT)] = (inb[p, :, cols(j, DT)].astype(F32) + v).astype(BF16)
            if jj == 0:
                g_out(i, 3, 1)
                start_d_out(i, 3, 1)

            @pl.when(jnp.logical_not(last))
            def _():
                for j in (2 * jj, 2 * jj + 1):
                    next_stage(k, i, j).start()

            @pl.when(last)
            def _():
                for j in (2 * jj, 2 * jj + 1):
                    for r in range(0, ROWS, 16):
                        diff = out[o, pl.ds(r, 16), cols(j, DT)].astype(F32) - inb[1 - p, pl.ds(r, 16), cols(j, DT)].astype(F32)
                        loss_acc[...] += diff * diff
                        inb[1 - p, pl.ds(r, 16), cols(j, DT)] = (diff * inv_total).astype(BF16)

        wait_d(2)

    def backward(k, i):
        p = lax.rem(k, 2)
        o = lax.rem(k, 2)

        def step1(j, carry):
            @pl.when(j == 0)
            def _():
                start_b1(2)
                start_b1(3)

            @pl.when((j >= 1) & jnp.logical_not(first))
            def _():
                start_b2(j - 1)

            @pl.when((j >= 1) & (j < 3) & first)
            def _():
                start_slot(k + 1, j - 1)

            @pl.when(j < NSTEP - 1)
            def _():
                start_d_in(i, j + 1)

            @pl.when((j == NSTEP - 1) & first)
            def _():
                before_next(k)

            wait_d(d_in_slot(j, 0))
            wait_d(d_in_slot(j, 1))
            wait_ring(j)
            pa = dot(inb[p], w2r[cols(j, CT), :], NT).astype(BF16).astype(F32)
            gq[:, d_cols(j, 0)] = (pa * dbuf[d_in_slot(j, 0)]).astype(BF16)
            pb = dot(inb[p, :, pl.ds(0, CT)], ring[j, pl.ds(0, CT)], NT)
            pb = pb + dot(inb[p, :, pl.ds(CT, CT)], ring[j, pl.ds(CT, CT)], NT)
            pb = pb.astype(BF16).astype(F32)
            gq[:, d_cols(j, 1)] = (pb * dbuf[d_in_slot(j, 1)]).astype(BF16)
            for b in range(2):
                copy(gq.at[:, d_cols(j, b)], qs.at[rows(i), d_cols(j, b)], gq_sem).start()
            return carry

        lax.fori_loop(0, NSTEP, step1, 0)
        wait_sent(k - 2)

        @pl.when(jnp.logical_not(first))
        def _():
            def step2(jj, carry):
                @pl.when(jj == 0)
                def _():
                    start_b2(3)

                @pl.when(jj == 1)
                def _():
                    start_slot(k + 1, 0)
                    start_slot(k + 1, 1)
                    before_next(k)

                for z in range(2):
                    wait_ring(2 * jj + z)
                for z in range(2):
                    j = 2 * jj + z
                    v = dot(gq[:, pl.ds(0, half)], w1r[cols(j, DT), :], NT)
                    for c in range(4):
                        v = v + dot(gq[:, pl.ds(half + c * CT, CT)], ring[j, pl.ds(c * DT, DT)], NT)
                    out[o, :, cols(j, DT)] = (inb[p, :, cols(j, DT)].astype(F32) + v).astype(BF16)
                for z in range(2):
                    prev_stage(k, i, 2 * jj + z).start()
                return carry

            lax.fori_loop(0, 2, step2, 0)

    def early_units(i):
        n_unit, after, each = early_plan(s)
        lo = jnp.clip((i - after) * each, 0, n_unit)
        return lo, jnp.where(i >= after, jnp.clip((i - after + 1) * each, 0, n_unit), lo)

    def early(i):
        lo, hi = early_units(i)
        n_tok = ring.shape[1]

        def tile(u, start):
            dst = ring.at[3, :, pl.ds(pl.multiple_of(lax.rem(u, 2) * DT, DT), DT)]
            sem = tile_sem.at[lax.rem(u, 2)]
            if not start:
                copy(dst, dst, sem).wait()
                return
            b = lax.rem(u, N_BLOCK)

            @pl.when(u < 2 * N_BLOCK)
            def _():
                copy(gs.at[pl.ds(0, n_tok), cols(b, DT)], dst, sem).start()

            @pl.when(u >= 2 * N_BLOCK)
            def _():
                copy(qs.at[pl.ds(0, n_tok), cols(b, DT)], dst, sem).start()

        def part_slot(t):
            z = lax.rem(t, 3)
            return jnp.where(z == 2, 4, z + 1)

        def wait_part(t):
            q = part_slot(t)
            copy(dbuf.at[q], dbuf.at[q], part_sem.at[lax.rem(t, 3)]).wait()

        def unit(u, carry):
            hf = lax.rem(u // N_BLOCK, 2)
            b = lax.rem(u, N_BLOCK)
            c0 = lax.rem(u, 2) * DT

            @pl.when((u == lo) | (b == 0))
            def _():
                @pl.when(u < 2 * N_BLOCK)
                def _():
                    copy(es.at[pl.ds(0, n_tok), cols(hf, CT)], ring.at[2], held_sem).start()

                @pl.when(u >= 2 * N_BLOCK)
                def _():
                    copy(hs.at[pl.ds(0, n_tok), cols(hf, CT)], ring.at[2], held_sem).start()

            @pl.when(u == lo)
            def _():
                tile(u, True)

            @pl.when(u + 1 < hi)
            def _():
                tile(u + 1, True)

            @pl.when((u == lo) | (b == 0))
            def _():
                copy(ring.at[2], ring.at[2], held_sem).wait()

            tile(u, False)
            for z in range(2):
                t = 2 * (u - lo) + z
                q = part_slot(t)

                @pl.when(t >= 3)
                def _():
                    wait_part(t)

                @pl.when(u < 2 * N_BLOCK)
                def _():
                    dbuf[q] = dot(ring[3, :, pl.ds(pl.multiple_of(c0 + z * ROWS, ROWS), ROWS)], ring[2], TN)
                    copy(dbuf.at[q], down_part.at[cols(2 * b + z, ROWS), cols(hf, CT)], part_sem.at[lax.rem(t, 3)]).start()

                @pl.when(u >= 2 * N_BLOCK)
                def _():
                    for a in range(2):
                        r = 2 * z + a
                        dbuf[q, :, pl.ds(a * DT, DT)] = dot(ring[2, :, pl.ds(r * ROWS, ROWS)], ring[3, :, pl.ds(pl.multiple_of(c0, DT), DT)], TN)
                    for a in range(2):
                        r = 2 * z + a
                        copy(dbuf.at[q, :, pl.ds(a * DT, DT)], up_part.at[cols(4 * hf + r, ROWS), cols(b, DT)], part_sem.at[lax.rem(t, 3)]).start()
            return carry

        lax.fori_loop(lo, hi, unit, 0)

        @pl.when(hi > lo)
        def _():
            wait_part(2 * (hi - lo) - 1)
            wait_part(2 * (hi - lo) - 2)

        @pl.when(hi > lo + 1)
        def _():
            wait_part(2 * (hi - lo) - 3)

    barrier = pltpu.get_barrier_semaphore()

    def hello(**to):
        pl.semaphore_signal(barrier, inc=1, device_id=to, device_id_type=pl.DeviceIdType.MESH)

    @pl.when(jnp.logical_not(first))
    def _():
        hello(stage=s - 1)

    @pl.when(jnp.logical_not(last))
    def _():
        hello(stage=s + 1)

    @pl.when(last)
    def _():
        hello(data=peer)

    @pl.when(first)
    def _():
        load_in(0)

    start_f1(0)
    for j in range(NSTEP):
        copy(w1.at[0, :, pl.ds(j * CT, CT)], w1r.at[:, pl.ds(j * CT, CT)], w1_sem.at[j]).start()
        if j == 0:
            start_f1(1)
    for j in range(NSTEP):
        copy(w2.at[0, pl.ds(0, half), pl.ds(j * DT, DT)], w2r.at[:, pl.ds(j * DT, DT)], w2_sem.at[j]).start()
    loss_acc[...] = jnp.zeros_like(loss_acc)

    @pl.when(first)
    def _():
        pl.semaphore_wait(barrier, 1)

    @pl.when(jnp.logical_not(first))
    def _():
        pl.semaphore_wait(barrier, 2)

    def slot(k, carry):
        is_f, i = order(k)
        p = lax.rem(k, 2)

        @pl.when(k > 0)
        def _():
            copy(gq, gq, gq_sem).wait()

        @pl.when(jnp.logical_not(ahead(k)))
        def _():
            load_in(k)

        @pl.when(needs_copy(k))
        def _():
            copy(inb.at[p], inb.at[p], in_sem.at[p]).wait()

        @pl.when(is_f & first)
        def _():
            copy(inb.at[p], hs.at[rows(i)], st_sem).start()

        @pl.when(jnp.logical_not(is_f) & last)
        def _():
            copy(inb.at[p], es.at[rows(i)], st_sem).start()

        @pl.when(is_f & last)
        def _():
            copy(y.at[rows(i)], inb.at[1 - p], y_sem).start()

        @pl.when(is_f)
        def _():
            forward(k, i)

        @pl.when(jnp.logical_not(is_f))
        def _():
            backward(k, i)

        @pl.when((is_f & first) | (jnp.logical_not(is_f) & last))
        def _():
            copy(inb.at[p], inb.at[p], st_sem).wait()

        @pl.when(jnp.logical_not(is_f))
        def _():
            early(i)

        return carry

    lax.fori_loop(0, n_slot, slot, 0)
    copy(gq, gq, gq_sem).wait()
    for k in range(n_slot - 2, n_slot):
        wait_sent(jnp.int32(k))

    def to_peer():
        return pltpu.make_async_remote_copy(
            src_ref=lbuf.at[0], dst_ref=lbuf.at[1], send_sem=l_send.at[0], recv_sem=l_recv.at[0],
            device_id={'data': peer}, device_id_type=pl.DeviceIdType.MESH)

    def to_prev():
        return pltpu.make_async_remote_copy(
            src_ref=lbuf.at[2], dst_ref=lbuf.at[2], send_sem=l_send.at[1], recv_sem=l_recv.at[1],
            device_id={'stage': s - 1}, device_id_type=pl.DeviceIdType.MESH)

    @pl.when(last)
    def _():
        lbuf[0] = loss_acc[pl.ds(0, 8), :] + loss_acc[pl.ds(8, 8), :]
        rdma = to_peer()
        rdma.start()
        rdma.wait()
        lbuf[2] = lbuf[0] + lbuf[1]

    @pl.when(jnp.logical_not(last))
    def _():
        copy(lbuf.at[2], lbuf.at[2], l_recv.at[1]).wait()

    loss_out[...] = lbuf[2]

    @pl.when(jnp.logical_not(first))
    def _():
        to_prev().start()
        copy(lbuf.at[2], lbuf.at[2], l_send.at[1]).wait()


def run_pipeline(n_stage, n_data, x, y, w1, w2):
    n_row, width = x.shape
    ffn = w1.shape[2]
    n_chunk = n_row // ROWS
    half = ffn // 2
    hbm = pl.BlockSpec(memory_space=pl.ANY)
    out = jax.ShapeDtypeStruct
    dma = pltpu.SemaphoreType.DMA
    flops = 8 * n_row * width * ffn
    return pl.pallas_call(
        functools.partial(pipeline_kernel, n_stage, n_data, n_chunk, 1.0 / (n_data * n_row)),
        out_shape=(out((n_row, width), BF16), out((n_row, ffn), BF16), out((n_row, ffn), F32),
                   out((n_row, ffn), BF16), out((n_row, width), BF16), out((width, ffn), F32), out((ffn, width), F32), out((8, DT), F32)),
        in_specs=[hbm] * 4,
        out_specs=(hbm,) * 7 + (pl.BlockSpec(memory_space=pltpu.VMEM),),
        scratch_shapes=[
            pltpu.VMEM((width, half), BF16), pltpu.VMEM((half, width), BF16),
            pltpu.VMEM((RING, width, CT), BF16), pltpu.VMEM((ROWS, ffn), BF16),
            pltpu.VMEM((5, ROWS, CT), F32), pltpu.VMEM((2, ROWS, width), BF16),
            pltpu.VMEM((2, ROWS, width), BF16), pltpu.VMEM((16, DT), F32),
            pltpu.VMEM((3, 8, DT), F32),
            dma((NSTEP,)), dma((NSTEP,)), dma((RING,)), dma((5,)), dma, dma((2,)), dma((2,)),
            dma((n_chunk,)), dma((n_chunk,)), dma, dma, dma((2,)), dma((2,)), dma, dma((2,)), dma((3,)),
        ],
        compiler_params=pltpu.CompilerParams(collective_id=0, has_side_effects=True, vmem_limit_bytes=67043328),
        cost_estimate=pl.CostEstimate(flops=flops, bytes_accessed=1 << 30, transcendentals=n_row * ffn),
        name='pipeline',
    )(x, y, w1, w2)


def grad_kernel(up, sc, held, lo, hi, part, *rest):
    got, o = rest if len(rest) == 2 else (None, rest[0])
    n = hi.shape[0]

    def product(rows_, tile):
        return dot(held[rows_, :], tile[...], TN) if up else dot(tile[...], held[rows_, :], TN)

    def finish(v):
        o[...] = v if got is None else v + got[...]

    @pl.when(pl.program_id(0) < sc[1])
    def _():
        finish(product(pl.ds(n, n), hi) + part[...])

    @pl.when(pl.program_id(0) >= sc[1])
    def _():
        finish(product(pl.ds(0, n), lo) + product(pl.ds(n, n), hi))


def weight_grad(up, held, streamed, part, side, n_done, got=None):
    n_row, width = held.shape
    half = width // 2
    n_tok = n_row // 2
    ffn = streamed.shape[1]
    shape = (half, DT) if up else (DT, half)

    def at(i, j):
        return (j, i) if up else (i, j)

    specs = [
        pl.BlockSpec((n_row, half), lambda b, sc: (0, sc[0])),
        pl.BlockSpec((n_tok, DT), lambda b, sc: (0, jnp.maximum(b, jnp.minimum(sc[1], N_BLOCK - 1)))),
        pl.BlockSpec((n_tok, DT), lambda b, sc: (1, b)),
        pl.BlockSpec(shape, lambda b, sc: at(jnp.minimum(b, jnp.maximum(sc[1] - 1, 0)), sc[0])),
    ]
    args = [held, streamed, streamed, part]
    if got is not None:
        specs.append(pl.BlockSpec(shape, lambda b, sc: at(b, 0)))
        args.append(got)
    return pl.pallas_call(
        functools.partial(grad_kernel, up),
        out_shape=jax.ShapeDtypeStruct((half, ffn) if up else (ffn, half), F32),
        grid_spec=pltpu.PrefetchScalarGridSpec(
            num_scalar_prefetch=1, grid=(ffn // DT,), in_specs=specs,
            out_specs=pl.BlockSpec(shape, lambda b, sc: at(b, 0))),
        compiler_params=pltpu.CompilerParams(dimension_semantics=('arbitrary',), vmem_limit_bytes=60 * 2**20),
        cost_estimate=pl.CostEstimate(flops=2 * n_row * half * ffn, bytes_accessed=2 * n_row * ffn + 8 * half * ffn, transcendentals=0),
        name='grad_up' if up else 'grad_down',
    )(jnp.stack([side, n_done]).astype(jnp.int32), *args)


def solution(mesh):
    n_stage = mesh.shape['stage']
    n_data = mesh.shape['data']

    def per_device(inputs, targets, w_up, w_down):
        n_micro, n_tok, width = inputs.shape
        n_row = n_micro * n_tok
        x = inputs.reshape(n_row, width)
        y = targets.reshape(n_row, width)
        hs, gs, _, qs, es, up_part, down_part, loss = run_pipeline(n_stage, n_data, x, y, w_up, w_down)
        n_unit, _, _ = early_plan(lax.axis_index('stage'))
        mine = lax.axis_index('data')
        other = n_data - 1 - mine
        swap = [(0, 1), (1, 0)]

        def grad(up, side, got=None):
            done = jnp.clip(n_unit - N_BLOCK * (side + (2 if up else 0)), 0, N_BLOCK)
            if up:
                return weight_grad(True, hs, qs, up_part, side, done, got)
            return weight_grad(False, es, gs, down_part, side, done, got)

        up_other = lax.ppermute(grad(True, other), 'data', swap)
        down_other = lax.ppermute(grad(False, other), 'data', swap)
        g_up = grad(True, mine, up_other)
        g_down = grad(False, mine, down_other)
        loss_total = jnp.sum(loss) * (0.5 / (n_data * n_row))
        return loss_total, g_up[None], g_down[None]

    return jax.shard_map(per_device, mesh=mesh, in_specs=(P('data', None, None), P('data', None, None), P('stage', None, None), P('stage', None, None)), out_specs=(P(), P('stage', 'data', None), P('stage', None, 'data')), check_vma=False)
```

```python
import functools

import jax
import jax.numpy as jnp
from jax import lax
from jax.experimental import pallas as pl
from jax.experimental.pallas import tpu as pltpu
from jax.sharding import PartitionSpec as P

BF16 = jnp.bfloat16
F32 = jnp.float32
C0 = 0.7978845608028654
C1 = 0.044715
ROWS = 256
CT = 1024
DT = 512
NSTEP = 4
RING = 4
NN = (((1,), (0,)), ((), ()))
NT = (((1,), (1,)), ((), ()))
TN = (((0,), (0,)), ((), ()))


def dot(a, b, dims):
    return lax.dot_general(a, b, dims, preferred_element_type=F32)


N_BLOCK = 16


def early_plan(s):
    n_unit = jnp.where(s == 0, 60, jnp.where(s == 1, 34, jnp.where(s == 2, 16, 0)))
    after = jnp.where(s == 2, 10, 8)
    each = jnp.where(s == 0, 60, jnp.where(s == 1, 6, 4))
    return n_unit, after, each


def pipeline_kernel(n_stage, n_data, n_chunk, inv_total,
                    x, y, w1, w2,
                    hs, gs, ds, qs, es, up_part, down_part, loss_out,
                    w1r, w2r, ring, gq, dbuf, inb, out, loss_acc, lbuf,
                    w1_sem, w2_sem, ring_sem, d_sem, gq_sem, in_sem, o_send,
                    h_recv, e_recv, y_sem, st_sem, l_send, l_recv, held_sem, tile_sem, part_sem):
    s = lax.axis_index('stage')
    peer = n_data - 1 - lax.axis_index('data')
    first = s == 0
    last = s == n_stage - 1
    half = w1r.shape[1]
    n_slot = 2 * n_chunk
    warm = jnp.where(first, n_chunk, jnp.where(last, 1, 12 - 4 * s))

    def order(k):
        j = jnp.maximum(k - warm, 0)
        left = n_chunk - warm
        early = k < warm
        mixed = j < 2 * left
        odd = lax.rem(j, 2) == 1
        is_f = early | (mixed & odd)
        idx = jnp.where(early, k, jnp.where(mixed, jnp.where(odd, warm + j // 2, j // 2), j - left))
        return is_f, idx

    def rows(i):
        return pl.ds(pl.multiple_of(i * ROWS, ROWS), ROWS)

    def cols(j, size, base=0):
        if isinstance(j, int):
            return pl.ds(base + j * size, size)
        return pl.ds(pl.multiple_of(base + j * size, size), size)

    def copy(src, dst, sem):
        return pltpu.make_async_copy(src, dst, sem)

    def start_f1(j):
        copy(w1.at[0, :, cols(j, CT, half)], ring.at[j], ring_sem.at[j]).start()

    def start_f2(j):
        for i in range(2):
            copy(w2.at[0, pl.ds(half + i * 2048, 2048), cols(j, DT)], ring.at[j, :, pl.ds(i * DT, DT)], ring_sem.at[j]).start()

    def start_b1(j):
        for i in range(2):
            copy(w2.at[0, cols(j, CT, half), pl.ds(i * CT, CT)], ring.at[j, pl.ds(i * CT, CT)], ring_sem.at[j]).start()

    def start_b2(j):
        for i in range(4):
            copy(w1.at[0, cols(j, DT), pl.ds(half + i * CT, CT)], ring.at[j, pl.ds(i * DT, DT)], ring_sem.at[j]).start()

    def start_slot(k, j):
        is_f, _ = order(k)

        @pl.when((k < n_slot) & is_f)
        def _():
            start_f1(j)

        @pl.when((k < n_slot) & jnp.logical_not(is_f))
        def _():
            start_b1(j)

    def wait_ring(r):
        copy(ring.at[r], ring.at[r], ring_sem.at[r]).wait()

    def d_cols(j, b):
        return cols(j, CT, b * half)

    def d_out_slot(j, b):
        return 2 + lax.rem(j, 3) if b else lax.rem(j, 2)

    def d_in_slot(j, b):
        return 3 * b + lax.rem(j, 2)

    def start_d_in(i, j):
        for b in range(2):
            copy(ds.at[rows(i), d_cols(j, b)], dbuf.at[d_in_slot(j, b)], d_sem.at[d_in_slot(j, b)]).start()

    def start_d_out(i, j, b):
        copy(dbuf.at[d_out_slot(j, b)], ds.at[rows(i), d_cols(j, b)], d_sem.at[d_out_slot(j, b)]).start()

    def wait_d(q):
        copy(dbuf.at[q], dbuf.at[q], d_sem.at[q]).wait()

    def needs_copy(k):
        is_f, _ = order(k)
        return is_f | jnp.logical_not(last)

    def ahead(k):
        return (first | (k >= warm)) & (k < n_slot)

    def load_in(k):
        is_f, i = order(k)
        b = lax.rem(k, 2)

        @pl.when(is_f & first)
        def _():
            copy(x.at[rows(i)], inb.at[b], in_sem.at[b]).start()

        @pl.when(is_f & jnp.logical_not(first))
        def _():
            copy(hs.at[rows(i)], hs.at[rows(i)], h_recv.at[i]).wait()
            copy(hs.at[rows(i)], inb.at[b], in_sem.at[b]).start()

        @pl.when(jnp.logical_not(is_f) & jnp.logical_not(last))
        def _():
            copy(es.at[rows(i)], es.at[rows(i)], e_recv.at[i]).wait()
            copy(es.at[rows(i)], inb.at[b], in_sem.at[b]).start()

    def before_next(k):
        is_f, i = order(k + 1)

        @pl.when(ahead(k + 1))
        def _():
            load_in(k + 1)

        @pl.when((k + 1 < n_slot) & jnp.logical_not(is_f))
        def _():
            start_d_in(i, 0)

    def next_stage(k, i, j):
        o = lax.rem(k, 2)
        return pltpu.make_async_remote_copy(
            src_ref=out.at[o, :, cols(j, DT)], dst_ref=hs.at[rows(i), cols(j, DT)],
            send_sem=o_send.at[o], recv_sem=h_recv.at[i],
            device_id={'stage': s + 1}, device_id_type=pl.DeviceIdType.MESH)

    def prev_stage(k, i, j):
        o = lax.rem(k, 2)
        return pltpu.make_async_remote_copy(
            src_ref=out.at[o, :, cols(j, DT)], dst_ref=es.at[rows(i), cols(j, DT)],
            send_sem=o_send.at[o], recv_sem=e_recv.at[i],
            device_id={'stage': s - 1}, device_id_type=pl.DeviceIdType.MESH)

    def sent(k):
        is_f, _ = order(k)
        return (is_f & jnp.logical_not(last)) | (jnp.logical_not(is_f) & jnp.logical_not(first))

    def wait_sent(k):
        @pl.when((k >= 0) & sent(jnp.maximum(k, 0)))
        def _():
            o = lax.rem(k, 2)
            copy(out.at[o], out.at[o], o_send.at[o]).wait()

    def gelu_tile(q, c, lo, hi):
        for r in range(0, ROWS, 16):
            for z in range(lo, hi, 256):
                u = dbuf[q, pl.ds(r, 16), pl.ds(z, 256)]
                u2 = u * u
                h = 0.5 * jnp.tanh(u * (C0 + (C0 * C1) * u2)) + 0.5
                g = u * h
                gq[pl.ds(r, 16), pl.ds(pl.multiple_of(c + z, 256), 256)] = g.astype(BF16)
                dbuf[q, pl.ds(r, 16), pl.ds(z, 256)] = h + (g * (1.0 - h)) * (2.0 * C0 + (6.0 * C0 * C1) * u2)

    def g_out(i, j, b):
        copy(gq.at[:, d_cols(j, b)], gs.at[rows(i), d_cols(j, b)], gq_sem).start()

    def forward(k, i):
        p = lax.rem(k, 2)
        o = lax.rem(k, 2)

        def step1(j, carry):
            @pl.when(j == 0)
            def _():
                start_f1(2)
                start_f1(3)

            @pl.when(j >= 1)
            def _():
                start_f2(j - 1)

            @pl.when(j >= 2)
            def _():
                wait_d(lax.rem(j, 2))

            @pl.when(j >= 3)
            def _():
                wait_d(2)

            @pl.when(k == 0)
            def _():
                copy(w1r.at[:, cols(j, CT)], w1r.at[:, cols(j, CT)], w1_sem.at[j]).wait()

            wait_ring(j)
            jp = jnp.maximum(j - 1, 0)
            res, stm, old = d_out_slot(j, 0), d_out_slot(j, 1), 2 + lax.rem(j + 2, 3)
            old_at, res_at = half + jp * CT, j * CT
            dbuf[res, :, pl.ds(0, DT)] = dot(inb[p], w1r[:, cols(2 * j, DT)], NN)
            gelu_tile(old, old_at, 0, 768)
            dbuf[res, :, pl.ds(DT, DT)] = dot(inb[p], w1r[:, cols(2 * j + 1, DT)], NN)
            gelu_tile(old, old_at, 768, CT)
            gelu_tile(res, res_at, 0, 512)
            dbuf[stm, :, pl.ds(0, DT)] = dot(inb[p], ring[j, :, pl.ds(0, DT)], NN)
            gelu_tile(res, res_at, 512, CT)
            dbuf[stm, :, pl.ds(DT, DT)] = dot(inb[p], ring[j, :, pl.ds(DT, DT)], NN)

            @pl.when(j >= 1)
            def _():
                g_out(i, j - 1, 1)
                start_d_out(i, j - 1, 1)

            g_out(i, j, 0)
            start_d_out(i, j, 0)
            return carry

        lax.fori_loop(0, NSTEP, step1, 0)

        @pl.when(last)
        def _():
            copy(inb.at[1 - p], inb.at[1 - p], y_sem).wait()

        wait_sent(k - 2)
        for jj in range(2):
            if jj == 0:
                start_f2(3)
                wait_d(3)
            else:
                start_slot(k + 1, 0)
                start_slot(k + 1, 1)
                for q in (0, 1, 4):
                    wait_d(q)
                before_next(k)

            @pl.when(k == 0)
            def _():
                for j in (2 * jj, 2 * jj + 1):
                    copy(w2r.at[:, cols(j, DT)], w2r.at[:, cols(j, DT)], w2_sem.at[j]).wait()

            for j in (2 * jj, 2 * jj + 1):
                wait_ring(j)
            for j in (2 * jj, 2 * jj + 1):
                v = dot(gq[:, pl.ds(0, half)], w2r[:, cols(j, DT)], NN)
                if j == 0:
                    dbuf[3, :, pl.ds(0, DT)] = v
                    gelu_tile(2, half + 3 * CT, 0, CT)
                    v = dbuf[3, :, pl.ds(0, DT)]
                v = v + dot(gq[:, pl.ds(half, 2048)], ring[j, :, pl.ds(0, DT)], NN)
                v = v + dot(gq[:, pl.ds(half + 2048, 2048)], ring[j, :, pl.ds(DT, DT)], NN)
                out[o, :, cols(j, DT)] = (inb[p, :, cols(j, DT)].astype(F32) + v).astype(BF16)
            if jj == 0:
                g_out(i, 3, 1)
                start_d_out(i, 3, 1)

            @pl.when(jnp.logical_not(last))
            def _():
                for j in (2 * jj, 2 * jj + 1):
                    next_stage(k, i, j).start()

            @pl.when(last)
            def _():
                for j in (2 * jj, 2 * jj + 1):
                    for r in range(0, ROWS, 16):
                        diff = out[o, pl.ds(r, 16), cols(j, DT)].astype(F32) - inb[1 - p, pl.ds(r, 16), cols(j, DT)].astype(F32)
                        loss_acc[...] += diff * diff
                        inb[1 - p, pl.ds(r, 16), cols(j, DT)] = (diff * inv_total).astype(BF16)

        wait_d(2)

    def backward(k, i):
        p = lax.rem(k, 2)
        o = lax.rem(k, 2)

        def step1(j, carry):
            @pl.when(j == 0)
            def _():
                start_b1(2)
                start_b1(3)

            @pl.when((j >= 1) & jnp.logical_not(first))
            def _():
                start_b2(j - 1)

            @pl.when((j >= 1) & (j < 3) & first)
            def _():
                start_slot(k + 1, j - 1)

            @pl.when(j < NSTEP - 1)
            def _():
                start_d_in(i, j + 1)

            @pl.when((j == NSTEP - 1) & first)
            def _():
                before_next(k)

            wait_d(d_in_slot(j, 0))
            wait_d(d_in_slot(j, 1))
            wait_ring(j)
            pa = dot(inb[p], w2r[cols(j, CT), :], NT).astype(BF16).astype(F32)
            gq[:, d_cols(j, 0)] = (pa * dbuf[d_in_slot(j, 0)]).astype(BF16)
            pb = dot(inb[p, :, pl.ds(0, CT)], ring[j, pl.ds(0, CT)], NT)
            pb = pb + dot(inb[p, :, pl.ds(CT, CT)], ring[j, pl.ds(CT, CT)], NT)
            pb = pb.astype(BF16).astype(F32)
            gq[:, d_cols(j, 1)] = (pb * dbuf[d_in_slot(j, 1)]).astype(BF16)
            for b in range(2):
                copy(gq.at[:, d_cols(j, b)], qs.at[rows(i), d_cols(j, b)], gq_sem).start()
            return carry

        lax.fori_loop(0, NSTEP, step1, 0)
        wait_sent(k - 2)

        @pl.when(jnp.logical_not(first))
        def _():
            def step2(jj, carry):
                @pl.when(jj == 0)
                def _():
                    start_b2(3)

                @pl.when(jj == 1)
                def _():
                    start_slot(k + 1, 0)
                    start_slot(k + 1, 1)
                    before_next(k)

                for z in range(2):
                    wait_ring(2 * jj + z)
                for z in range(2):
                    j = 2 * jj + z
                    v = dot(gq[:, pl.ds(0, half)], w1r[cols(j, DT), :], NT)
                    for c in range(4):
                        v = v + dot(gq[:, pl.ds(half + c * CT, CT)], ring[j, pl.ds(c * DT, DT)], NT)
                    out[o, :, cols(j, DT)] = (inb[p, :, cols(j, DT)].astype(F32) + v).astype(BF16)
                for z in range(2):
                    prev_stage(k, i, 2 * jj + z).start()
                return carry

            lax.fori_loop(0, 2, step2, 0)

    def early_units(i):
        n_unit, after, each = early_plan(s)
        lo = jnp.clip((i - after) * each, 0, n_unit)
        return lo, jnp.where(i >= after, jnp.clip((i - after + 1) * each, 0, n_unit), lo)

    def early(i):
        lo, hi = early_units(i)
        n_tok = ring.shape[1]

        def tile(u, start):
            dst = ring.at[3, :, pl.ds(pl.multiple_of(lax.rem(u, 2) * DT, DT), DT)]
            sem = tile_sem.at[lax.rem(u, 2)]
            if not start:
                copy(dst, dst, sem).wait()
                return
            b = lax.rem(u, N_BLOCK)

            @pl.when(u < 2 * N_BLOCK)
            def _():
                copy(gs.at[pl.ds(0, n_tok), cols(b, DT)], dst, sem).start()

            @pl.when(u >= 2 * N_BLOCK)
            def _():
                copy(qs.at[pl.ds(0, n_tok), cols(b, DT)], dst, sem).start()

        def part_slot(t):
            z = lax.rem(t, 3)
            return jnp.where(z == 2, 4, z + 1)

        def wait_part(t):
            q = part_slot(t)
            copy(dbuf.at[q], dbuf.at[q], part_sem.at[lax.rem(t, 3)]).wait()

        def unit(u, carry):
            hf = lax.rem(u // N_BLOCK, 2)
            b = lax.rem(u, N_BLOCK)
            c0 = lax.rem(u, 2) * DT

            @pl.when((u == lo) | (b == 0))
            def _():
                @pl.when(u < 2 * N_BLOCK)
                def _():
                    copy(es.at[pl.ds(0, n_tok), cols(hf, CT)], ring.at[2], held_sem).start()

                @pl.when(u >= 2 * N_BLOCK)
                def _():
                    copy(hs.at[pl.ds(0, n_tok), cols(hf, CT)], ring.at[2], held_sem).start()

            @pl.when(u == lo)
            def _():
                tile(u, True)

            @pl.when(u + 1 < hi)
            def _():
                tile(u + 1, True)

            @pl.when((u == lo) | (b == 0))
            def _():
                copy(ring.at[2], ring.at[2], held_sem).wait()

            tile(u, False)
            for z in range(2):
                t = 2 * (u - lo) + z
                q = part_slot(t)

                @pl.when(t >= 3)
                def _():
                    wait_part(t)

                @pl.when(u < 2 * N_BLOCK)
                def _():
                    dbuf[q] = dot(ring[3, :, pl.ds(pl.multiple_of(c0 + z * ROWS, ROWS), ROWS)], ring[2], TN)
                    copy(dbuf.at[q], down_part.at[cols(2 * b + z, ROWS), cols(hf, CT)], part_sem.at[lax.rem(t, 3)]).start()

                @pl.when(u >= 2 * N_BLOCK)
                def _():
                    for a in range(2):
                        r = 2 * z + a
                        dbuf[q, :, pl.ds(a * DT, DT)] = dot(ring[2, :, pl.ds(r * ROWS, ROWS)], ring[3, :, pl.ds(pl.multiple_of(c0, DT), DT)], TN)
                    for a in range(2):
                        r = 2 * z + a
                        copy(dbuf.at[q, :, pl.ds(a * DT, DT)], up_part.at[cols(4 * hf + r, ROWS), cols(b, DT)], part_sem.at[lax.rem(t, 3)]).start()
            return carry

        lax.fori_loop(lo, hi, unit, 0)

        @pl.when(hi > lo)
        def _():
            wait_part(2 * (hi - lo) - 1)
            wait_part(2 * (hi - lo) - 2)

        @pl.when(hi > lo + 1)
        def _():
            wait_part(2 * (hi - lo) - 3)

    barrier = pltpu.get_barrier_semaphore()

    def hello(**to):
        pl.semaphore_signal(barrier, inc=1, device_id=to, device_id_type=pl.DeviceIdType.MESH)

    @pl.when(jnp.logical_not(first))
    def _():
        hello(stage=s - 1)

    @pl.when(jnp.logical_not(last))
    def _():
        hello(stage=s + 1)

    @pl.when(last)
    def _():
        hello(data=peer)

    @pl.when(first)
    def _():
        load_in(0)

    start_f1(0)
    for j in range(NSTEP):
        copy(w1.at[0, :, pl.ds(j * CT, CT)], w1r.at[:, pl.ds(j * CT, CT)], w1_sem.at[j]).start()
        if j == 0:
            start_f1(1)
    for j in range(NSTEP):
        copy(w2.at[0, pl.ds(0, half), pl.ds(j * DT, DT)], w2r.at[:, pl.ds(j * DT, DT)], w2_sem.at[j]).start()
    loss_acc[...] = jnp.zeros_like(loss_acc)

    @pl.when(first)
    def _():
        pl.semaphore_wait(barrier, 1)

    @pl.when(jnp.logical_not(first))
    def _():
        pl.semaphore_wait(barrier, 2)

    def slot(k, carry):
        is_f, i = order(k)
        p = lax.rem(k, 2)

        @pl.when(k > 0)
        def _():
            copy(gq, gq, gq_sem).wait()

        @pl.when(jnp.logical_not(ahead(k)))
        def _():
            load_in(k)

        @pl.when(needs_copy(k))
        def _():
            copy(inb.at[p], inb.at[p], in_sem.at[p]).wait()

        @pl.when(is_f & first)
        def _():
            copy(inb.at[p], hs.at[rows(i)], st_sem).start()

        @pl.when(jnp.logical_not(is_f) & last)
        def _():
            copy(inb.at[p], es.at[rows(i)], st_sem).start()

        @pl.when(is_f & last)
        def _():
            copy(y.at[rows(i)], inb.at[1 - p], y_sem).start()

        @pl.when(is_f)
        def _():
            forward(k, i)

        @pl.when(jnp.logical_not(is_f))
        def _():
            backward(k, i)

        @pl.when((is_f & first) | (jnp.logical_not(is_f) & last))
        def _():
            copy(inb.at[p], inb.at[p], st_sem).wait()

        @pl.when(jnp.logical_not(is_f))
        def _():
            early(i)

        return carry

    lax.fori_loop(0, n_slot, slot, 0)
    copy(gq, gq, gq_sem).wait()
    for k in range(n_slot - 2, n_slot):
        wait_sent(jnp.int32(k))

    def to_peer():
        return pltpu.make_async_remote_copy(
            src_ref=lbuf.at[0], dst_ref=lbuf.at[1], send_sem=l_send.at[0], recv_sem=l_recv.at[0],
            device_id={'data': peer}, device_id_type=pl.DeviceIdType.MESH)

    def to_prev():
        return pltpu.make_async_remote_copy(
            src_ref=lbuf.at[2], dst_ref=lbuf.at[2], send_sem=l_send.at[1], recv_sem=l_recv.at[1],
            device_id={'stage': s - 1}, device_id_type=pl.DeviceIdType.MESH)

    @pl.when(last)
    def _():
        lbuf[0] = loss_acc[pl.ds(0, 8), :] + loss_acc[pl.ds(8, 8), :]
        rdma = to_peer()
        rdma.start()
        rdma.wait()
        lbuf[2] = lbuf[0] + lbuf[1]

    @pl.when(jnp.logical_not(last))
    def _():
        copy(lbuf.at[2], lbuf.at[2], l_recv.at[1]).wait()

    loss_out[...] = lbuf[2]

    @pl.when(jnp.logical_not(first))
    def _():
        to_prev().start()
        copy(lbuf.at[2], lbuf.at[2], l_send.at[1]).wait()


def run_pipeline(n_stage, n_data, x, y, w1, w2):
    n_row, width = x.shape
    ffn = w1.shape[2]
    n_chunk = n_row // ROWS
    half = ffn // 2
    hbm = pl.BlockSpec(memory_space=pl.ANY)
    out = jax.ShapeDtypeStruct
    dma = pltpu.SemaphoreType.DMA
    flops = 8 * n_row * width * ffn
    return pl.pallas_call(
        functools.partial(pipeline_kernel, n_stage, n_data, n_chunk, 1.0 / (n_data * n_row)),
        out_shape=(out((n_row, width), BF16), out((n_row, ffn), BF16), out((n_row, ffn), F32),
                   out((n_row, ffn), BF16), out((n_row, width), BF16), out((width, ffn), F32), out((ffn, width), F32), out((8, DT), F32)),
        in_specs=[hbm] * 4,
        out_specs=(hbm,) * 7 + (pl.BlockSpec(memory_space=pltpu.VMEM),),
        scratch_shapes=[
            pltpu.VMEM((width, half), BF16), pltpu.VMEM((half, width), BF16),
            pltpu.VMEM((RING, width, CT), BF16), pltpu.VMEM((ROWS, ffn), BF16),
            pltpu.VMEM((5, ROWS, CT), F32), pltpu.VMEM((2, ROWS, width), BF16),
            pltpu.VMEM((2, ROWS, width), BF16), pltpu.VMEM((16, DT), F32),
            pltpu.VMEM((3, 8, DT), F32),
            dma((NSTEP,)), dma((NSTEP,)), dma((RING,)), dma((5,)), dma, dma((2,)), dma((2,)),
            dma((n_chunk,)), dma((n_chunk,)), dma, dma, dma((2,)), dma((2,)), dma, dma((2,)), dma((3,)),
        ],
        compiler_params=pltpu.CompilerParams(collective_id=0, has_side_effects=True, vmem_limit_bytes=67043328),
        cost_estimate=pl.CostEstimate(flops=flops, bytes_accessed=1 << 30, transcendentals=n_row * ffn),
        name='pipeline',
    )(x, y, w1, w2)


def grad_kernel(up, sc, held, lo, hi, part, *rest):
    got, o = rest if len(rest) == 2 else (None, rest[0])
    n = hi.shape[0]

    def product(rows_, tile):
        return dot(held[rows_, :], tile[...], TN) if up else dot(tile[...], held[rows_, :], TN)

    def finish(v):
        o[...] = v if got is None else v + got[...]

    @pl.when(pl.program_id(0) < sc[1])
    def _():
        finish(product(pl.ds(n, n), hi) + part[...])

    @pl.when(pl.program_id(0) >= sc[1])
    def _():
        finish(product(pl.ds(0, n), lo) + product(pl.ds(n, n), hi))


def weight_grad(up, held, streamed, part, side, n_done, got=None):
    n_row, width = held.shape
    half = width // 2
    n_tok = n_row // 2
    ffn = streamed.shape[1]
    shape = (half, DT) if up else (DT, half)

    def at(i, j):
        return (j, i) if up else (i, j)

    specs = [
        pl.BlockSpec((n_row, half), lambda b, sc: (0, sc[0])),
        pl.BlockSpec((n_tok, DT), lambda b, sc: (0, jnp.maximum(b, jnp.minimum(sc[1], N_BLOCK - 1)))),
        pl.BlockSpec((n_tok, DT), lambda b, sc: (1, b)),
        pl.BlockSpec(shape, lambda b, sc: at(jnp.minimum(b, jnp.maximum(sc[1] - 1, 0)), sc[0])),
    ]
    args = [held, streamed, streamed, part]
    if got is not None:
        specs.append(pl.BlockSpec(shape, lambda b, sc: at(b, 0)))
        args.append(got)
    return pl.pallas_call(
        functools.partial(grad_kernel, up),
        out_shape=jax.ShapeDtypeStruct((half, ffn) if up else (ffn, half), F32),
        grid_spec=pltpu.PrefetchScalarGridSpec(
            num_scalar_prefetch=1, grid=(ffn // DT,), in_specs=specs,
            out_specs=pl.BlockSpec(shape, lambda b, sc: at(b, 0))),
        compiler_params=pltpu.CompilerParams(dimension_semantics=('arbitrary',), vmem_limit_bytes=60 * 2**20),
        cost_estimate=pl.CostEstimate(flops=2 * n_row * half * ffn, bytes_accessed=2 * n_row * ffn + 8 * half * ffn, transcendentals=0),
        name='grad_up' if up else 'grad_down',
    )(jnp.stack([side, n_done]).astype(jnp.int32), *args)


def solution(mesh):
    n_stage = mesh.shape['stage']
    n_data = mesh.shape['data']

    def per_device(inputs, targets, w_up, w_down):
        n_micro, n_tok, width = inputs.shape
        n_row = n_micro * n_tok
        x = inputs.reshape(n_row, width)
        y = targets.reshape(n_row, width)
        hs, gs, _, qs, es, up_part, down_part, loss = run_pipeline(n_stage, n_data, x, y, w_up, w_down)
        n_unit, _, _ = early_plan(lax.axis_index('stage'))
        mine = lax.axis_index('data')
        other = n_data - 1 - mine
        swap = [(0, 1), (1, 0)]

        def grad(up, side, got=None):
            done = jnp.clip(n_unit - N_BLOCK * (side + (2 if up else 0)), 0, N_BLOCK)
            if up:
                return weight_grad(True, hs, qs, up_part, side, done, got)
            return weight_grad(False, es, gs, down_part, side, done, got)

        up_other = lax.ppermute(grad(True, other), 'data', swap)
        down_other = lax.ppermute(grad(False, other), 'data', swap)
        g_up = grad(True, mine, up_other)
        g_down = grad(False, mine, down_other)
        loss_total = jnp.sum(loss) * (0.5 / (n_data * n_row))
        return loss_total, g_up[None], g_down[None]

    return jax.shard_map(per_device, mesh=mesh, in_specs=(P('data', None, None), P('data', None, None), P('stage', None, None), P('stage', None, None)), out_specs=(P(), P('stage', 'data', None), P('stage', None, 'data')), check_vma=False)
```

```python
import functools

import jax
import jax.numpy as jnp
from jax import lax
from jax.experimental import pallas as pl
from jax.experimental.pallas import tpu as pltpu
from jax.sharding import PartitionSpec as P

BF16 = jnp.bfloat16
F32 = jnp.float32
C0 = 0.7978845608028654
C1 = 0.044715
ROWS = 256
CT = 1024
DT = 512
NSTEP = 4
RING = 4
NN = (((1,), (0,)), ((), ()))
NT = (((1,), (1,)), ((), ()))
TN = (((0,), (0,)), ((), ()))


def dot(a, b, dims):
    return lax.dot_general(a, b, dims, preferred_element_type=F32)


N_BLOCK = 16


def early_plan(s):
    n_unit = jnp.where(s == 0, 60, jnp.where(s == 1, 32, jnp.where(s == 2, 16, 0)))
    after = jnp.where(s == 2, 10, jnp.where(s == 1, 7, 8))
    each = jnp.where(s == 0, 60, jnp.where(s == 1, 5, 4))
    return n_unit, after, each


def pipeline_kernel(n_stage, n_data, n_chunk, inv_total,
                    x, y, w1, w2,
                    hs, gs, ds, qs, es, up_part, down_part, loss_out,
                    w1r, w2r, ring, gq, dbuf, inb, out, loss_acc, lbuf,
                    w1_sem, w2_sem, ring_sem, d_sem, gq_sem, in_sem, o_send,
                    h_recv, e_recv, y_sem, st_sem, l_send, l_recv, held_sem, tile_sem, part_sem):
    s = lax.axis_index('stage')
    peer = n_data - 1 - lax.axis_index('data')
    first = s == 0
    last = s == n_stage - 1
    half = w1r.shape[1]
    n_slot = 2 * n_chunk
    warm = jnp.where(first, n_chunk, jnp.where(last, 1, 12 - 4 * s))

    def order(k):
        j = jnp.maximum(k - warm, 0)
        left = n_chunk - warm
        early = k < warm
        mixed = j < 2 * left
        odd = lax.rem(j, 2) == 1
        is_f = early | (mixed & odd)
        idx = jnp.where(early, k, jnp.where(mixed, jnp.where(odd, warm + j // 2, j // 2), j - left))
        return is_f, idx

    def rows(i):
        return pl.ds(pl.multiple_of(i * ROWS, ROWS), ROWS)

    def cols(j, size, base=0):
        if isinstance(j, int):
            return pl.ds(base + j * size, size)
        return pl.ds(pl.multiple_of(base + j * size, size), size)

    def copy(src, dst, sem):
        return pltpu.make_async_copy(src, dst, sem)

    def start_f1(j):
        copy(w1.at[0, :, cols(j, CT, half)], ring.at[j], ring_sem.at[j]).start()

    def start_f2(j):
        for i in range(2):
            copy(w2.at[0, pl.ds(half + i * 2048, 2048), cols(j, DT)], ring.at[j, :, pl.ds(i * DT, DT)], ring_sem.at[j]).start()

    def start_b1(j):
        for i in range(2):
            copy(w2.at[0, cols(j, CT, half), pl.ds(i * CT, CT)], ring.at[j, pl.ds(i * CT, CT)], ring_sem.at[j]).start()

    def start_b2(j):
        for i in range(4):
            copy(w1.at[0, cols(j, DT), pl.ds(half + i * CT, CT)], ring.at[j, pl.ds(i * DT, DT)], ring_sem.at[j]).start()

    def start_slot(k, j):
        is_f, _ = order(k)

        @pl.when((k < n_slot) & is_f)
        def _():
            start_f1(j)

        @pl.when((k < n_slot) & jnp.logical_not(is_f))
        def _():
            start_b1(j)

    def wait_ring(r):
        copy(ring.at[r], ring.at[r], ring_sem.at[r]).wait()

    def d_cols(j, b):
        return cols(j, CT, b * half)

    def d_out_slot(j, b):
        return 2 + lax.rem(j, 3) if b else lax.rem(j, 2)

    def d_in_slot(j, b):
        return 3 * b + lax.rem(j, 2)

    def start_d_in(i, j):
        for b in range(2):
            copy(ds.at[rows(i), d_cols(j, b)], dbuf.at[d_in_slot(j, b)], d_sem.at[d_in_slot(j, b)]).start()

    def start_d_out(i, j, b):
        copy(dbuf.at[d_out_slot(j, b)], ds.at[rows(i), d_cols(j, b)], d_sem.at[d_out_slot(j, b)]).start()

    def wait_d(q):
        copy(dbuf.at[q], dbuf.at[q], d_sem.at[q]).wait()

    def needs_copy(k):
        is_f, _ = order(k)
        return is_f | jnp.logical_not(last)

    def ahead(k):
        is_f, _ = order(k)
        return is_f & (first | (last & (k >= warm))) & (k < n_slot)

    def load_in(k):
        is_f, i = order(k)
        b = lax.rem(k, 2)

        @pl.when(is_f & first)
        def _():
            copy(x.at[rows(i)], inb.at[b], in_sem.at[b]).start()

        @pl.when(is_f & jnp.logical_not(first))
        def _():
            copy(hs.at[rows(i)], hs.at[rows(i)], h_recv.at[i]).wait()
            copy(hs.at[rows(i)], inb.at[b], in_sem.at[b]).start()

        @pl.when(jnp.logical_not(is_f) & jnp.logical_not(last))
        def _():
            copy(es.at[rows(i)], es.at[rows(i)], e_recv.at[i]).wait()
            copy(es.at[rows(i)], inb.at[b], in_sem.at[b]).start()

    def before_next(k):
        is_f, i = order(k + 1)

        @pl.when(ahead(k + 1))
        def _():
            load_in(k + 1)

        @pl.when((k + 1 < n_slot) & jnp.logical_not(is_f))
        def _():
            start_d_in(i, 0)

    def next_stage(k, i, j):
        o = lax.rem(k, 2)
        return pltpu.make_async_remote_copy(
            src_ref=out.at[o, :, cols(j, DT)], dst_ref=hs.at[rows(i), cols(j, DT)],
            send_sem=o_send.at[o], recv_sem=h_recv.at[i],
            device_id={'stage': s + 1}, device_id_type=pl.DeviceIdType.MESH)

    def prev_stage(k, i, j):
        o = lax.rem(k, 2)
        return pltpu.make_async_remote_copy(
            src_ref=out.at[o, :, cols(j, DT)], dst_ref=es.at[rows(i), cols(j, DT)],
            send_sem=o_send.at[o], recv_sem=e_recv.at[i],
            device_id={'stage': s - 1}, device_id_type=pl.DeviceIdType.MESH)

    def sent(k):
        is_f, _ = order(k)
        return (is_f & jnp.logical_not(last)) | (jnp.logical_not(is_f) & jnp.logical_not(first))

    def wait_sent(k):
        @pl.when((k >= 0) & sent(jnp.maximum(k, 0)))
        def _():
            o = lax.rem(k, 2)
            copy(out.at[o], out.at[o], o_send.at[o]).wait()

    def gelu_tile(q, c, lo, hi):
        for r in range(0, ROWS, 16):
            for z in range(lo, hi, 256):
                u = dbuf[q, pl.ds(r, 16), pl.ds(z, 256)]
                u2 = u * u
                h = 0.5 * jnp.tanh(u * (C0 + (C0 * C1) * u2)) + 0.5
                g = u * h
                gq[pl.ds(r, 16), pl.ds(pl.multiple_of(c + z, 256), 256)] = g.astype(BF16)
                dbuf[q, pl.ds(r, 16), pl.ds(z, 256)] = h + (g * (1.0 - h)) * (2.0 * C0 + (6.0 * C0 * C1) * u2)

    def g_out(i, j, b):
        copy(gq.at[:, d_cols(j, b)], gs.at[rows(i), d_cols(j, b)], gq_sem).start()

    def forward(k, i):
        p = lax.rem(k, 2)
        o = lax.rem(k, 2)

        def step1(j, carry):
            @pl.when(j == 0)
            def _():
                start_f1(2)
                start_f1(3)

            @pl.when(j >= 1)
            def _():
                start_f2(j - 1)

            @pl.when(j >= 2)
            def _():
                wait_d(lax.rem(j, 2))

            @pl.when(j >= 3)
            def _():
                wait_d(2)

            @pl.when(k == 0)
            def _():
                copy(w1r.at[:, cols(j, CT)], w1r.at[:, cols(j, CT)], w1_sem.at[j]).wait()

            wait_ring(j)
            jp = jnp.maximum(j - 1, 0)
            res, stm, old = d_out_slot(j, 0), d_out_slot(j, 1), 2 + lax.rem(j + 2, 3)
            old_at, res_at = half + jp * CT, j * CT
            dbuf[res, :, pl.ds(0, DT)] = dot(inb[p], w1r[:, cols(2 * j, DT)], NN)
            gelu_tile(old, old_at, 0, 768)
            dbuf[res, :, pl.ds(DT, DT)] = dot(inb[p], w1r[:, cols(2 * j + 1, DT)], NN)
            gelu_tile(old, old_at, 768, CT)
            gelu_tile(res, res_at, 0, 512)
            dbuf[stm, :, pl.ds(0, DT)] = dot(inb[p], ring[j, :, pl.ds(0, DT)], NN)
            gelu_tile(res, res_at, 512, CT)
            dbuf[stm, :, pl.ds(DT, DT)] = dot(inb[p], ring[j, :, pl.ds(DT, DT)], NN)

            @pl.when(j >= 1)
            def _():
                g_out(i, j - 1, 1)
                start_d_out(i, j - 1, 1)

            g_out(i, j, 0)
            start_d_out(i, j, 0)
            return carry

        lax.fori_loop(0, NSTEP, step1, 0)

        @pl.when(last)
        def _():
            copy(inb.at[1 - p], inb.at[1 - p], y_sem).wait()

        wait_sent(k - 2)
        for jj in range(2):
            if jj == 0:
                start_f2(3)
                wait_d(3)
            else:
                start_slot(k + 1, 0)
                start_slot(k + 1, 1)
                for q in (0, 1, 4):
                    wait_d(q)
                before_next(k)

            @pl.when(k == 0)
            def _():
                for j in (2 * jj, 2 * jj + 1):
                    copy(w2r.at[:, cols(j, DT)], w2r.at[:, cols(j, DT)], w2_sem.at[j]).wait()

            for j in (2 * jj, 2 * jj + 1):
                wait_ring(j)
            for j in (2 * jj, 2 * jj + 1):
                v = dot(gq[:, pl.ds(0, half)], w2r[:, cols(j, DT)], NN)
                if j == 0:
                    dbuf[3, :, pl.ds(0, DT)] = v
                    gelu_tile(2, half + 3 * CT, 0, CT)
                    v = dbuf[3, :, pl.ds(0, DT)]
                v = v + dot(gq[:, pl.ds(half, 2048)], ring[j, :, pl.ds(0, DT)], NN)
                v = v + dot(gq[:, pl.ds(half + 2048, 2048)], ring[j, :, pl.ds(DT, DT)], NN)
                out[o, :, cols(j, DT)] = (inb[p, :, cols(j, DT)].astype(F32) + v).astype(BF16)
            if jj == 0:
                g_out(i, 3, 1)
                start_d_out(i, 3, 1)

            @pl.when(jnp.logical_not(last))
            def _():
                for j in (2 * jj, 2 * jj + 1):
                    next_stage(k, i, j).start()

            @pl.when(last)
            def _():
                for j in (2 * jj, 2 * jj + 1):
                    for r in range(0, ROWS, 16):
                        diff = out[o, pl.ds(r, 16), cols(j, DT)].astype(F32) - inb[1 - p, pl.ds(r, 16), cols(j, DT)].astype(F32)
                        loss_acc[...] += diff * diff
                        inb[1 - p, pl.ds(r, 16), cols(j, DT)] = (diff * inv_total).astype(BF16)

        wait_d(2)

    def backward(k, i):
        p = lax.rem(k, 2)
        o = lax.rem(k, 2)

        def step1(j, carry):
            @pl.when(j == 0)
            def _():
                start_b1(2)
                start_b1(3)

            @pl.when((j >= 1) & jnp.logical_not(first))
            def _():
                start_b2(j - 1)

            @pl.when((j >= 1) & (j < 3) & first)
            def _():
                start_slot(k + 1, j - 1)

            @pl.when(j < NSTEP - 1)
            def _():
                start_d_in(i, j + 1)

            @pl.when((j == NSTEP - 1) & first)
            def _():
                before_next(k)

            wait_d(d_in_slot(j, 0))
            wait_d(d_in_slot(j, 1))
            wait_ring(j)
            pa = dot(inb[p], w2r[cols(j, CT), :], NT).astype(BF16).astype(F32)
            gq[:, d_cols(j, 0)] = (pa * dbuf[d_in_slot(j, 0)]).astype(BF16)
            pb = dot(inb[p, :, pl.ds(0, CT)], ring[j, pl.ds(0, CT)], NT)
            pb = pb + dot(inb[p, :, pl.ds(CT, CT)], ring[j, pl.ds(CT, CT)], NT)
            pb = pb.astype(BF16).astype(F32)
            gq[:, d_cols(j, 1)] = (pb * dbuf[d_in_slot(j, 1)]).astype(BF16)
            for b in range(2):
                copy(gq.at[:, d_cols(j, b)], qs.at[rows(i), d_cols(j, b)], gq_sem).start()
            return carry

        lax.fori_loop(0, NSTEP, step1, 0)
        wait_sent(k - 2)

        @pl.when(jnp.logical_not(first))
        def _():
            def step2(jj, carry):
                @pl.when(jj == 0)
                def _():
                    start_b2(3)

                @pl.when(jj == 1)
                def _():
                    start_slot(k + 1, 0)
                    start_slot(k + 1, 1)
                    before_next(k)

                for z in range(2):
                    wait_ring(2 * jj + z)
                for z in range(2):
                    j = 2 * jj + z
                    v = dot(gq[:, pl.ds(0, half)], w1r[cols(j, DT), :], NT)
                    for c in range(4):
                        v = v + dot(gq[:, pl.ds(half + c * CT, CT)], ring[j, pl.ds(c * DT, DT)], NT)
                    out[o, :, cols(j, DT)] = (inb[p, :, cols(j, DT)].astype(F32) + v).astype(BF16)
                for z in range(2):
                    prev_stage(k, i, 2 * jj + z).start()
                return carry

            lax.fori_loop(0, 2, step2, 0)

    def early_units(i):
        n_unit, after, each = early_plan(s)
        lo = jnp.clip((i - after) * each, 0, n_unit)
        return lo, jnp.where(i >= after, jnp.clip((i - after + 1) * each, 0, n_unit), lo)

    def early(i):
        lo, hi = early_units(i)
        n_tok = ring.shape[1]

        def tile(u, start):
            dst = ring.at[3, :, pl.ds(pl.multiple_of(lax.rem(u, 2) * DT, DT), DT)]
            sem = tile_sem.at[lax.rem(u, 2)]
            if not start:
                copy(dst, dst, sem).wait()
                return
            b = lax.rem(u, N_BLOCK)

            @pl.when(u < 2 * N_BLOCK)
            def _():
                copy(gs.at[pl.ds(0, n_tok), cols(b, DT)], dst, sem).start()

            @pl.when(u >= 2 * N_BLOCK)
            def _():
                copy(qs.at[pl.ds(0, n_tok), cols(b, DT)], dst, sem).start()

        def part_slot(t):
            z = lax.rem(t, 3)
            return jnp.where(z == 2, 4, z + 1)

        def wait_part(t):
            q = part_slot(t)
            copy(dbuf.at[q], dbuf.at[q], part_sem.at[lax.rem(t, 3)]).wait()

        def unit(u, carry):
            hf = lax.rem(u // N_BLOCK, 2)
            b = lax.rem(u, N_BLOCK)
            c0 = lax.rem(u, 2) * DT

            @pl.when((u == lo) | (b == 0))
            def _():
                @pl.when(u < 2 * N_BLOCK)
                def _():
                    copy(es.at[pl.ds(0, n_tok), cols(hf, CT)], ring.at[2], held_sem).start()

                @pl.when(u >= 2 * N_BLOCK)
                def _():
                    copy(hs.at[pl.ds(0, n_tok), cols(hf, CT)], ring.at[2], held_sem).start()

            @pl.when(u == lo)
            def _():
                tile(u, True)

            @pl.when(u + 1 < hi)
            def _():
                tile(u + 1, True)

            @pl.when((u == lo) | (b == 0))
            def _():
                copy(ring.at[2], ring.at[2], held_sem).wait()

            tile(u, False)
            for z in range(2):
                t = 2 * (u - lo) + z
                q = part_slot(t)

                @pl.when(t >= 3)
                def _():
                    wait_part(t)

                @pl.when(u < 2 * N_BLOCK)
                def _():
                    dbuf[q] = dot(ring[3, :, pl.ds(pl.multiple_of(c0 + z * ROWS, ROWS), ROWS)], ring[2], TN)
                    copy(dbuf.at[q], down_part.at[cols(2 * b + z, ROWS), cols(hf, CT)], part_sem.at[lax.rem(t, 3)]).start()

                @pl.when(u >= 2 * N_BLOCK)
                def _():
                    for a in range(2):
                        r = 2 * z + a
                        dbuf[q, :, pl.ds(a * DT, DT)] = dot(ring[2, :, pl.ds(r * ROWS, ROWS)], ring[3, :, pl.ds(pl.multiple_of(c0, DT), DT)], TN)
                    for a in range(2):
                        r = 2 * z + a
                        copy(dbuf.at[q, :, pl.ds(a * DT, DT)], up_part.at[cols(4 * hf + r, ROWS), cols(b, DT)], part_sem.at[lax.rem(t, 3)]).start()
            return carry

        lax.fori_loop(lo, hi, unit, 0)

        @pl.when(hi > lo)
        def _():
            wait_part(2 * (hi - lo) - 1)
            wait_part(2 * (hi - lo) - 2)

        @pl.when(hi > lo + 1)
        def _():
            wait_part(2 * (hi - lo) - 3)

    barrier = pltpu.get_barrier_semaphore()

    def hello(**to):
        pl.semaphore_signal(barrier, inc=1, device_id=to, device_id_type=pl.DeviceIdType.MESH)

    @pl.when(jnp.logical_not(first))
    def _():
        hello(stage=s - 1)

    @pl.when(jnp.logical_not(last))
    def _():
        hello(stage=s + 1)

    @pl.when(last)
    def _():
        hello(data=peer)

    @pl.when(first)
    def _():
        load_in(0)

    start_f1(0)
    for j in range(NSTEP):
        copy(w1.at[0, :, pl.ds(j * CT, CT)], w1r.at[:, pl.ds(j * CT, CT)], w1_sem.at[j]).start()
        if j == 0:
            start_f1(1)
    for j in range(NSTEP):
        copy(w2.at[0, pl.ds(0, half), pl.ds(j * DT, DT)], w2r.at[:, pl.ds(j * DT, DT)], w2_sem.at[j]).start()
    loss_acc[...] = jnp.zeros_like(loss_acc)

    @pl.when(first)
    def _():
        pl.semaphore_wait(barrier, 1)

    @pl.when(jnp.logical_not(first))
    def _():
        pl.semaphore_wait(barrier, 2)

    def slot(k, carry):
        is_f, i = order(k)
        p = lax.rem(k, 2)

        @pl.when(k > 0)
        def _():
            copy(gq, gq, gq_sem).wait()

        @pl.when(jnp.logical_not(ahead(k)))
        def _():
            load_in(k)

        @pl.when(needs_copy(k))
        def _():
            copy(inb.at[p], inb.at[p], in_sem.at[p]).wait()

        @pl.when(is_f & first)
        def _():
            copy(inb.at[p], hs.at[rows(i)], st_sem).start()

        @pl.when(jnp.logical_not(is_f) & last)
        def _():
            copy(inb.at[p], es.at[rows(i)], st_sem).start()

        @pl.when(is_f & last)
        def _():
            copy(y.at[rows(i)], inb.at[1 - p], y_sem).start()

        @pl.when(is_f)
        def _():
            forward(k, i)

        @pl.when(jnp.logical_not(is_f))
        def _():
            backward(k, i)

        @pl.when((is_f & first) | (jnp.logical_not(is_f) & last))
        def _():
            copy(inb.at[p], inb.at[p], st_sem).wait()

        @pl.when(jnp.logical_not(is_f))
        def _():
            early(i)

        return carry

    lax.fori_loop(0, n_slot, slot, 0)
    copy(gq, gq, gq_sem).wait()
    for k in range(n_slot - 2, n_slot):
        wait_sent(jnp.int32(k))

    def to_peer():
        return pltpu.make_async_remote_copy(
            src_ref=lbuf.at[0], dst_ref=lbuf.at[1], send_sem=l_send.at[0], recv_sem=l_recv.at[0],
            device_id={'data': peer}, device_id_type=pl.DeviceIdType.MESH)

    def to_prev():
        return pltpu.make_async_remote_copy(
            src_ref=lbuf.at[2], dst_ref=lbuf.at[2], send_sem=l_send.at[1], recv_sem=l_recv.at[1],
            device_id={'stage': s - 1}, device_id_type=pl.DeviceIdType.MESH)

    @pl.when(last)
    def _():
        lbuf[0] = loss_acc[pl.ds(0, 8), :] + loss_acc[pl.ds(8, 8), :]
        rdma = to_peer()
        rdma.start()
        rdma.wait()
        lbuf[2] = lbuf[0] + lbuf[1]

    @pl.when(jnp.logical_not(last))
    def _():
        copy(lbuf.at[2], lbuf.at[2], l_recv.at[1]).wait()

    loss_out[...] = lbuf[2]

    @pl.when(jnp.logical_not(first))
    def _():
        to_prev().start()
        copy(lbuf.at[2], lbuf.at[2], l_send.at[1]).wait()


def run_pipeline(n_stage, n_data, x, y, w1, w2):
    n_row, width = x.shape
    ffn = w1.shape[2]
    n_chunk = n_row // ROWS
    half = ffn // 2
    hbm = pl.BlockSpec(memory_space=pl.ANY)
    out = jax.ShapeDtypeStruct
    dma = pltpu.SemaphoreType.DMA
    flops = 8 * n_row * width * ffn
    return pl.pallas_call(
        functools.partial(pipeline_kernel, n_stage, n_data, n_chunk, 1.0 / (n_data * n_row)),
        out_shape=(out((n_row, width), BF16), out((n_row, ffn), BF16), out((n_row, ffn), F32),
                   out((n_row, ffn), BF16), out((n_row, width), BF16), out((width, ffn), F32), out((ffn, width), F32), out((8, DT), F32)),
        in_specs=[hbm] * 4,
        out_specs=(hbm,) * 7 + (pl.BlockSpec(memory_space=pltpu.VMEM),),
        scratch_shapes=[
            pltpu.VMEM((width, half), BF16), pltpu.VMEM((half, width), BF16),
            pltpu.VMEM((RING, width, CT), BF16), pltpu.VMEM((ROWS, ffn), BF16),
            pltpu.VMEM((5, ROWS, CT), F32), pltpu.VMEM((2, ROWS, width), BF16),
            pltpu.VMEM((2, ROWS, width), BF16), pltpu.VMEM((16, DT), F32),
            pltpu.VMEM((3, 8, DT), F32),
            dma((NSTEP,)), dma((NSTEP,)), dma((RING,)), dma((5,)), dma, dma((2,)), dma((2,)),
            dma((n_chunk,)), dma((n_chunk,)), dma, dma, dma((2,)), dma((2,)), dma, dma((2,)), dma((3,)),
        ],
        compiler_params=pltpu.CompilerParams(collective_id=0, has_side_effects=True, vmem_limit_bytes=67043328),
        cost_estimate=pl.CostEstimate(flops=flops, bytes_accessed=1 << 30, transcendentals=n_row * ffn),
        name='pipeline',
    )(x, y, w1, w2)


def grad_kernel(up, sc, held, lo, hi, part, *rest):
    got, o = rest if len(rest) == 2 else (None, rest[0])
    n = hi.shape[0]

    def product(rows_, tile):
        return dot(held[rows_, :], tile[...], TN) if up else dot(tile[...], held[rows_, :], TN)

    def finish(v):
        o[...] = v if got is None else v + got[...]

    @pl.when(pl.program_id(0) < sc[1])
    def _():
        finish(product(pl.ds(n, n), hi) + part[...])

    @pl.when(pl.program_id(0) >= sc[1])
    def _():
        finish(product(pl.ds(0, n), lo) + product(pl.ds(n, n), hi))


def weight_grad(up, held, streamed, part, side, n_done, got=None):
    n_row, width = held.shape
    half = width // 2
    n_tok = n_row // 2
    ffn = streamed.shape[1]
    shape = (half, DT) if up else (DT, half)

    def at(i, j):
        return (j, i) if up else (i, j)

    specs = [
        pl.BlockSpec((n_row, half), lambda b, sc: (0, sc[0])),
        pl.BlockSpec((n_tok, DT), lambda b, sc: (0, jnp.maximum(b, jnp.minimum(sc[1], N_BLOCK - 1)))),
        pl.BlockSpec((n_tok, DT), lambda b, sc: (1, b)),
        pl.BlockSpec(shape, lambda b, sc: at(jnp.minimum(b, jnp.maximum(sc[1] - 1, 0)), sc[0])),
    ]
    args = [held, streamed, streamed, part]
    if got is not None:
        specs.append(pl.BlockSpec(shape, lambda b, sc: at(b, 0)))
        args.append(got)
    return pl.pallas_call(
        functools.partial(grad_kernel, up),
        out_shape=jax.ShapeDtypeStruct((half, ffn) if up else (ffn, half), F32),
        grid_spec=pltpu.PrefetchScalarGridSpec(
            num_scalar_prefetch=1, grid=(ffn // DT,), in_specs=specs,
            out_specs=pl.BlockSpec(shape, lambda b, sc: at(b, 0))),
        compiler_params=pltpu.CompilerParams(dimension_semantics=('arbitrary',), vmem_limit_bytes=60 * 2**20),
        cost_estimate=pl.CostEstimate(flops=2 * n_row * half * ffn, bytes_accessed=2 * n_row * ffn + 8 * half * ffn, transcendentals=0),
        name='grad_up' if up else 'grad_down',
    )(jnp.stack([side, n_done]).astype(jnp.int32), *args)


def solution(mesh):
    n_stage = mesh.shape['stage']
    n_data = mesh.shape['data']

    def per_device(inputs, targets, w_up, w_down):
        n_micro, n_tok, width = inputs.shape
        n_row = n_micro * n_tok
        x = inputs.reshape(n_row, width)
        y = targets.reshape(n_row, width)
        hs, gs, _, qs, es, up_part, down_part, loss = run_pipeline(n_stage, n_data, x, y, w_up, w_down)
        n_unit, _, _ = early_plan(lax.axis_index('stage'))
        mine = lax.axis_index('data')
        other = n_data - 1 - mine
        swap = [(0, 1), (1, 0)]

        def grad(up, side, got=None):
            done = jnp.clip(n_unit - N_BLOCK * (side + (2 if up else 0)), 0, N_BLOCK)
            if up:
                return weight_grad(True, hs, qs, up_part, side, done, got)
            return weight_grad(False, es, gs, down_part, side, done, got)

        up_other = lax.ppermute(grad(True, other), 'data', swap)
        down_other = lax.ppermute(grad(False, other), 'data', swap)
        g_up = grad(True, mine, up_other)
        g_down = grad(False, mine, down_other)
        loss_total = jnp.sum(loss) * (0.5 / (n_data * n_row))
        return loss_total, g_up[None], g_down[None]

    return jax.shard_map(per_device, mesh=mesh, in_specs=(P('data', None, None), P('data', None, None), P('stage', None, None), P('stage', None, None)), out_specs=(P(), P('stage', 'data', None), P('stage', None, 'data')), check_vma=False)
```

```python
import functools

import jax
import jax.numpy as jnp
from jax import lax
from jax.experimental import pallas as pl
from jax.experimental.pallas import tpu as pltpu
from jax.sharding import PartitionSpec as P

BF16 = jnp.bfloat16
F32 = jnp.float32
C0 = 0.7978845608028654
C1 = 0.044715
ROWS = 256
CT = 1024
DT = 512
NSTEP = 4
RING = 4
NN = (((1,), (0,)), ((), ()))
NT = (((1,), (1,)), ((), ()))
TN = (((0,), (0,)), ((), ()))


def dot(a, b, dims):
    return lax.dot_general(a, b, dims, preferred_element_type=F32)


N_BLOCK = 16


def early_plan(s):
    n_down = jnp.where(s < 2, N_BLOCK, jnp.where(s == 2, 6, 0))
    n_up = jnp.where(s == 0, 14, 0)
    after = jnp.where(s == 2, 12, 8)
    each = jnp.where(s == 0, 60, jnp.where(s == 1, 5, 4))
    return n_down, n_up, after, each


def pipeline_kernel(n_stage, n_data, n_chunk, inv_total,
                    x, y, w1, w2,
                    hs, gs, ds, qs, es, up_part, down_part, loss_out,
                    w1r, w2r, ring, gq, dbuf, inb, out, loss_acc, lbuf,
                    w1_sem, w2_sem, ring_sem, d_sem, gq_sem, in_sem, o_send,
                    h_recv, e_recv, y_sem, st_sem, l_send, l_recv, held_sem, tile_sem, part_sem):
    s = lax.axis_index('stage')
    peer = n_data - 1 - lax.axis_index('data')
    first = s == 0
    last = s == n_stage - 1
    half = w1r.shape[1]
    n_slot = 2 * n_chunk
    warm = jnp.where(first, n_chunk, jnp.where(last, 1, 12 - 4 * s))

    def order(k):
        j = jnp.maximum(k - warm, 0)
        left = n_chunk - warm
        early = k < warm
        mixed = j < 2 * left
        odd = lax.rem(j, 2) == 1
        is_f = early | (mixed & odd)
        idx = jnp.where(early, k, jnp.where(mixed, jnp.where(odd, warm + j // 2, j // 2), j - left))
        return is_f, idx

    def rows(i):
        return pl.ds(pl.multiple_of(i * ROWS, ROWS), ROWS)

    def cols(j, size, base=0):
        if isinstance(j, int):
            return pl.ds(base + j * size, size)
        return pl.ds(pl.multiple_of(base + j * size, size), size)

    def copy(src, dst, sem):
        return pltpu.make_async_copy(src, dst, sem)

    def start_f1(j):
        copy(w1.at[0, :, cols(j, CT, half)], ring.at[j], ring_sem.at[j]).start()

    def start_f2(j):
        for i in range(2):
            copy(w2.at[0, pl.ds(half + i * 2048, 2048), cols(j, DT)], ring.at[j, :, pl.ds(i * DT, DT)], ring_sem.at[j]).start()

    def start_b1(j):
        for i in range(2):
            copy(w2.at[0, cols(j, CT, half), pl.ds(i * CT, CT)], ring.at[j, pl.ds(i * CT, CT)], ring_sem.at[j]).start()

    def start_b2(j):
        for i in range(4):
            copy(w1.at[0, cols(j, DT), pl.ds(half + i * CT, CT)], ring.at[j, pl.ds(i * DT, DT)], ring_sem.at[j]).start()

    def start_slot(k, j):
        is_f, _ = order(k)

        @pl.when((k < n_slot) & is_f)
        def _():
            start_f1(j)

        @pl.when((k < n_slot) & jnp.logical_not(is_f))
        def _():
            start_b1(j)

    def wait_ring(r):
        copy(ring.at[r], ring.at[r], ring_sem.at[r]).wait()

    def d_cols(j, b):
        return cols(j, CT, b * half)

    def d_out_slot(j, b):
        return 2 + lax.rem(j, 3) if b else lax.rem(j, 2)

    def d_in_slot(j, b):
        return 3 * b + lax.rem(j, 2)

    def start_d_in(i, j):
        for b in range(2):
            copy(ds.at[rows(i), d_cols(j, b)], dbuf.at[d_in_slot(j, b)], d_sem.at[d_in_slot(j, b)]).start()

    def start_d_out(i, j, b):
        copy(dbuf.at[d_out_slot(j, b)], ds.at[rows(i), d_cols(j, b)], d_sem.at[d_out_slot(j, b)]).start()

    def wait_d(q):
        copy(dbuf.at[q], dbuf.at[q], d_sem.at[q]).wait()

    def needs_copy(k):
        is_f, _ = order(k)
        return is_f | jnp.logical_not(last)

    def ahead(k):
        is_f, _ = order(k)
        return is_f & (first | (last & (k >= warm))) & (k < n_slot)

    def load_in(k):
        is_f, i = order(k)
        b = lax.rem(k, 2)

        @pl.when(is_f & first)
        def _():
            copy(x.at[rows(i)], inb.at[b], in_sem.at[b]).start()

        @pl.when(is_f & jnp.logical_not(first))
        def _():
            copy(hs.at[rows(i)], hs.at[rows(i)], h_recv.at[i]).wait()
            copy(hs.at[rows(i)], inb.at[b], in_sem.at[b]).start()

        @pl.when(jnp.logical_not(is_f) & jnp.logical_not(last))
        def _():
            copy(es.at[rows(i)], es.at[rows(i)], e_recv.at[i]).wait()
            copy(es.at[rows(i)], inb.at[b], in_sem.at[b]).start()

    def before_next(k):
        is_f, i = order(k + 1)

        @pl.when(ahead(k + 1))
        def _():
            load_in(k + 1)

        @pl.when((k + 1 < n_slot) & jnp.logical_not(is_f))
        def _():
            start_d_in(i, 0)

    def next_stage(k, i, j):
        o = lax.rem(k, 2)
        return pltpu.make_async_remote_copy(
            src_ref=out.at[o, :, cols(j, DT)], dst_ref=hs.at[rows(i), cols(j, DT)],
            send_sem=o_send.at[o], recv_sem=h_recv.at[i],
            device_id={'stage': s + 1}, device_id_type=pl.DeviceIdType.MESH)

    def prev_stage(k, i, j):
        o = lax.rem(k, 2)
        return pltpu.make_async_remote_copy(
            src_ref=out.at[o, :, cols(j, DT)], dst_ref=es.at[rows(i), cols(j, DT)],
            send_sem=o_send.at[o], recv_sem=e_recv.at[i],
            device_id={'stage': s - 1}, device_id_type=pl.DeviceIdType.MESH)

    def sent(k):
        is_f, _ = order(k)
        return (is_f & jnp.logical_not(last)) | (jnp.logical_not(is_f) & jnp.logical_not(first))

    def wait_sent(k):
        @pl.when((k >= 0) & sent(jnp.maximum(k, 0)))
        def _():
            o = lax.rem(k, 2)
            copy(out.at[o], out.at[o], o_send.at[o]).wait()

    def gelu_tile(q, c, lo, hi):
        for r in range(0, ROWS, 16):
            for z in range(lo, hi, 256):
                u = dbuf[q, pl.ds(r, 16), pl.ds(z, 256)]
                u2 = u * u
                h = 0.5 * jnp.tanh(u * (C0 + (C0 * C1) * u2)) + 0.5
                g = u * h
                gq[pl.ds(r, 16), pl.ds(pl.multiple_of(c + z, 256), 256)] = g.astype(BF16)
                dbuf[q, pl.ds(r, 16), pl.ds(z, 256)] = h + (g * (1.0 - h)) * (2.0 * C0 + (6.0 * C0 * C1) * u2)

    def g_out(i, j, b):
        copy(gq.at[:, d_cols(j, b)], gs.at[rows(i), d_cols(j, b)], gq_sem).start()

    def forward(k, i):
        p = lax.rem(k, 2)
        o = lax.rem(k, 2)

        def step1(j, carry):
            @pl.when(j == 0)
            def _():
                start_f1(2)
                start_f1(3)

            @pl.when(j >= 1)
            def _():
                start_f2(j - 1)

            @pl.when(j >= 2)
            def _():
                wait_d(lax.rem(j, 2))

            @pl.when(j >= 3)
            def _():
                wait_d(2)

            @pl.when(k == 0)
            def _():
                copy(w1r.at[:, cols(j, CT)], w1r.at[:, cols(j, CT)], w1_sem.at[j]).wait()

            wait_ring(j)
            jp = jnp.maximum(j - 1, 0)
            res, stm, old = d_out_slot(j, 0), d_out_slot(j, 1), 2 + lax.rem(j + 2, 3)
            old_at, res_at = half + jp * CT, j * CT
            dbuf[res, :, pl.ds(0, DT)] = dot(inb[p], w1r[:, cols(2 * j, DT)], NN)
            gelu_tile(old, old_at, 0, 768)
            dbuf[res, :, pl.ds(DT, DT)] = dot(inb[p], w1r[:, cols(2 * j + 1, DT)], NN)
            gelu_tile(old, old_at, 768, CT)
            gelu_tile(res, res_at, 0, 512)
            dbuf[stm, :, pl.ds(0, DT)] = dot(inb[p], ring[j, :, pl.ds(0, DT)], NN)
            gelu_tile(res, res_at, 512, CT)
            dbuf[stm, :, pl.ds(DT, DT)] = dot(inb[p], ring[j, :, pl.ds(DT, DT)], NN)

            @pl.when(j >= 1)
            def _():
                g_out(i, j - 1, 1)
                start_d_out(i, j - 1, 1)

            g_out(i, j, 0)
            start_d_out(i, j, 0)
            return carry

        lax.fori_loop(0, NSTEP, step1, 0)

        @pl.when(last)
        def _():
            copy(inb.at[1 - p], inb.at[1 - p], y_sem).wait()

        wait_sent(k - 2)
        for jj in range(2):
            if jj == 0:
                start_f2(3)
                wait_d(3)
            else:
                start_slot(k + 1, 0)
                start_slot(k + 1, 1)
                for q in (0, 1, 4):
                    wait_d(q)
                before_next(k)

            @pl.when(k == 0)
            def _():
                for j in (2 * jj, 2 * jj + 1):
                    copy(w2r.at[:, cols(j, DT)], w2r.at[:, cols(j, DT)], w2_sem.at[j]).wait()

            for j in (2 * jj, 2 * jj + 1):
                wait_ring(j)
            for j in (2 * jj, 2 * jj + 1):
                v = dot(gq[:, pl.ds(0, half)], w2r[:, cols(j, DT)], NN)
                if j == 0:
                    dbuf[3, :, pl.ds(0, DT)] = v
                    gelu_tile(2, half + 3 * CT, 0, CT)
                    v = dbuf[3, :, pl.ds(0, DT)]
                v = v + dot(gq[:, pl.ds(half, 2048)], ring[j, :, pl.ds(0, DT)], NN)
                v = v + dot(gq[:, pl.ds(half + 2048, 2048)], ring[j, :, pl.ds(DT, DT)], NN)
                out[o, :, cols(j, DT)] = (inb[p, :, cols(j, DT)].astype(F32) + v).astype(BF16)
            if jj == 0:
                g_out(i, 3, 1)
                start_d_out(i, 3, 1)

            @pl.when(jnp.logical_not(last))
            def _():
                for j in (2 * jj, 2 * jj + 1):
                    next_stage(k, i, j).start()

            @pl.when(last)
            def _():
                for j in (2 * jj, 2 * jj + 1):
                    for r in range(0, ROWS, 16):
                        diff = out[o, pl.ds(r, 16), cols(j, DT)].astype(F32) - inb[1 - p, pl.ds(r, 16), cols(j, DT)].astype(F32)
                        loss_acc[...] += diff * diff
                        inb[1 - p, pl.ds(r, 16), cols(j, DT)] = (diff * inv_total).astype(BF16)

        wait_d(2)

    def backward(k, i):
        p = lax.rem(k, 2)
        o = lax.rem(k, 2)

        def step1(j, carry):
            @pl.when(j == 0)
            def _():
                start_b1(2)
                start_b1(3)

            @pl.when((j >= 1) & jnp.logical_not(first))
            def _():
                start_b2(j - 1)

            @pl.when((j >= 1) & (j < 3) & first)
            def _():
                start_slot(k + 1, j - 1)

            @pl.when(j < NSTEP - 1)
            def _():
                start_d_in(i, j + 1)

            @pl.when((j == NSTEP - 1) & first)
            def _():
                before_next(k)

            wait_d(d_in_slot(j, 0))
            wait_d(d_in_slot(j, 1))
            wait_ring(j)
            pa = dot(inb[p], w2r[cols(j, CT), :], NT).astype(BF16).astype(F32)
            gq[:, d_cols(j, 0)] = (pa * dbuf[d_in_slot(j, 0)]).astype(BF16)
            pb = dot(inb[p, :, pl.ds(0, CT)], ring[j, pl.ds(0, CT)], NT)
            pb = pb + dot(inb[p, :, pl.ds(CT, CT)], ring[j, pl.ds(CT, CT)], NT)
            pb = pb.astype(BF16).astype(F32)
            gq[:, d_cols(j, 1)] = (pb * dbuf[d_in_slot(j, 1)]).astype(BF16)
            for b in range(2):
                copy(gq.at[:, d_cols(j, b)], qs.at[rows(i), d_cols(j, b)], gq_sem).start()
            return carry

        lax.fori_loop(0, NSTEP, step1, 0)
        wait_sent(k - 2)

        @pl.when(jnp.logical_not(first))
        def _():
            def step2(jj, carry):
                @pl.when(jj == 0)
                def _():
                    start_b2(3)

                @pl.when(jj == 1)
                def _():
                    start_slot(k + 1, 0)
                    start_slot(k + 1, 1)
                    before_next(k)

                for z in range(2):
                    wait_ring(2 * jj + z)
                for z in range(2):
                    j = 2 * jj + z
                    v = dot(gq[:, pl.ds(0, half)], w1r[cols(j, DT), :], NT)
                    for c in range(4):
                        v = v + dot(gq[:, pl.ds(half + c * CT, CT)], ring[j, pl.ds(c * DT, DT)], NT)
                    out[o, :, cols(j, DT)] = (inb[p, :, cols(j, DT)].astype(F32) + v).astype(BF16)
                for z in range(2):
                    prev_stage(k, i, 2 * jj + z).start()
                return carry

            lax.fori_loop(0, 2, step2, 0)

    def early_units(i):
        n_down, n_up, after, each = early_plan(s)
        n_unit = 2 * (n_down + n_up)
        lo = jnp.clip((i - after) * each, 0, n_unit)
        return lo, jnp.where(i >= after, jnp.clip((i - after + 1) * each, 0, n_unit), lo)

    def early(i):
        lo, hi = early_units(i)
        n_tok = ring.shape[1]
        n_down, n_up, _, _ = early_plan(s)

        def place(u):
            down = u < 2 * n_down
            v = jnp.where(down, u, u - 2 * n_down)
            n = jnp.maximum(jnp.where(down, n_down, n_up), 1)
            side = jnp.where(v >= n, 1, 0)
            return down, side, v - n * side


        def tile(u, start):
            dst = ring.at[3, :, pl.ds(pl.multiple_of(lax.rem(u, 2) * DT, DT), DT)]
            sem = tile_sem.at[lax.rem(u, 2)]
            if not start:
                copy(dst, dst, sem).wait()
                return
            down, _, b = place(u)

            @pl.when(down)
            def _():
                copy(gs.at[pl.ds(0, n_tok), cols(b, DT)], dst, sem).start()

            @pl.when(jnp.logical_not(down))
            def _():
                copy(qs.at[pl.ds(0, n_tok), cols(b, DT)], dst, sem).start()

        def part_slot(t):
            z = lax.rem(t, 3)
            return jnp.where(z == 2, 4, z + 1)

        def wait_part(t):
            q = part_slot(t)
            copy(dbuf.at[q], dbuf.at[q], part_sem.at[lax.rem(t, 3)]).wait()

        def unit(u, carry):
            down, hf, b = place(u)
            c0 = lax.rem(u, 2) * DT

            @pl.when((u == lo) | (b == 0))
            def _():
                @pl.when(down)
                def _():
                    copy(es.at[pl.ds(0, n_tok), cols(hf, CT)], ring.at[2], held_sem).start()

                @pl.when(jnp.logical_not(down))
                def _():
                    copy(hs.at[pl.ds(0, n_tok), cols(hf, CT)], ring.at[2], held_sem).start()

            @pl.when(u == lo)
            def _():
                tile(u, True)

            @pl.when(u + 1 < hi)
            def _():
                tile(u + 1, True)

            @pl.when((u == lo) | (b == 0))
            def _():
                copy(ring.at[2], ring.at[2], held_sem).wait()

            tile(u, False)
            for z in range(2):
                t = 2 * (u - lo) + z
                q = part_slot(t)

                @pl.when(t >= 3)
                def _():
                    wait_part(t)

                @pl.when(down)
                def _():
                    dbuf[q] = dot(ring[3, :, pl.ds(pl.multiple_of(c0 + z * ROWS, ROWS), ROWS)], ring[2], TN)
                    copy(dbuf.at[q], down_part.at[cols(2 * b + z, ROWS), cols(hf, CT)], part_sem.at[lax.rem(t, 3)]).start()

                @pl.when(jnp.logical_not(down))
                def _():
                    for a in range(2):
                        r = 2 * z + a
                        dbuf[q, :, pl.ds(a * DT, DT)] = dot(ring[2, :, pl.ds(r * ROWS, ROWS)], ring[3, :, pl.ds(pl.multiple_of(c0, DT), DT)], TN)
                    for a in range(2):
                        r = 2 * z + a
                        copy(dbuf.at[q, :, pl.ds(a * DT, DT)], up_part.at[cols(4 * hf + r, ROWS), cols(b, DT)], part_sem.at[lax.rem(t, 3)]).start()
            return carry

        lax.fori_loop(lo, hi, unit, 0)

        @pl.when(hi > lo)
        def _():
            wait_part(2 * (hi - lo) - 1)
            wait_part(2 * (hi - lo) - 2)

        @pl.when(hi > lo + 1)
        def _():
            wait_part(2 * (hi - lo) - 3)

    barrier = pltpu.get_barrier_semaphore()

    def hello(**to):
        pl.semaphore_signal(barrier, inc=1, device_id=to, device_id_type=pl.DeviceIdType.MESH)

    @pl.when(jnp.logical_not(first))
    def _():
        hello(stage=s - 1)

    @pl.when(jnp.logical_not(last))
    def _():
        hello(stage=s + 1)

    @pl.when(last)
    def _():
        hello(data=peer)

    @pl.when(first)
    def _():
        load_in(0)

    start_f1(0)
    for j in range(NSTEP):
        copy(w1.at[0, :, pl.ds(j * CT, CT)], w1r.at[:, pl.ds(j * CT, CT)], w1_sem.at[j]).start()
        if j == 0:
            start_f1(1)
    for j in range(NSTEP):
        copy(w2.at[0, pl.ds(0, half), pl.ds(j * DT, DT)], w2r.at[:, pl.ds(j * DT, DT)], w2_sem.at[j]).start()
    loss_acc[...] = jnp.zeros_like(loss_acc)

    @pl.when(first)
    def _():
        pl.semaphore_wait(barrier, 1)

    @pl.when(jnp.logical_not(first))
    def _():
        pl.semaphore_wait(barrier, 2)

    def slot(k, carry):
        is_f, i = order(k)
        p = lax.rem(k, 2)

        @pl.when(k > 0)
        def _():
            copy(gq, gq, gq_sem).wait()

        @pl.when(jnp.logical_not(ahead(k)))
        def _():
            load_in(k)

        @pl.when(needs_copy(k))
        def _():
            copy(inb.at[p], inb.at[p], in_sem.at[p]).wait()

        @pl.when(is_f & first)
        def _():
            copy(inb.at[p], hs.at[rows(i)], st_sem).start()

        @pl.when(jnp.logical_not(is_f) & last)
        def _():
            copy(inb.at[p], es.at[rows(i)], st_sem).start()

        @pl.when(is_f & last)
        def _():
            copy(y.at[rows(i)], inb.at[1 - p], y_sem).start()

        @pl.when(is_f)
        def _():
            forward(k, i)

        @pl.when(jnp.logical_not(is_f))
        def _():
            backward(k, i)

        @pl.when((is_f & first) | (jnp.logical_not(is_f) & last))
        def _():
            copy(inb.at[p], inb.at[p], st_sem).wait()

        @pl.when(jnp.logical_not(is_f))
        def _():
            early(i)

        return carry

    lax.fori_loop(0, n_slot, slot, 0)
    copy(gq, gq, gq_sem).wait()
    for k in range(n_slot - 2, n_slot):
        wait_sent(jnp.int32(k))

    def to_peer():
        return pltpu.make_async_remote_copy(
            src_ref=lbuf.at[0], dst_ref=lbuf.at[1], send_sem=l_send.at[0], recv_sem=l_recv.at[0],
            device_id={'data': peer}, device_id_type=pl.DeviceIdType.MESH)

    def to_prev():
        return pltpu.make_async_remote_copy(
            src_ref=lbuf.at[2], dst_ref=lbuf.at[2], send_sem=l_send.at[1], recv_sem=l_recv.at[1],
            device_id={'stage': s - 1}, device_id_type=pl.DeviceIdType.MESH)

    @pl.when(last)
    def _():
        lbuf[0] = loss_acc[pl.ds(0, 8), :] + loss_acc[pl.ds(8, 8), :]
        rdma = to_peer()
        rdma.start()
        rdma.wait()
        lbuf[2] = lbuf[0] + lbuf[1]

    @pl.when(jnp.logical_not(last))
    def _():
        copy(lbuf.at[2], lbuf.at[2], l_recv.at[1]).wait()

    loss_out[...] = lbuf[2]

    @pl.when(jnp.logical_not(first))
    def _():
        to_prev().start()
        copy(lbuf.at[2], lbuf.at[2], l_send.at[1]).wait()


def run_pipeline(n_stage, n_data, x, y, w1, w2):
    n_row, width = x.shape
    ffn = w1.shape[2]
    n_chunk = n_row // ROWS
    half = ffn // 2
    hbm = pl.BlockSpec(memory_space=pl.ANY)
    out = jax.ShapeDtypeStruct
    dma = pltpu.SemaphoreType.DMA
    flops = 8 * n_row * width * ffn
    return pl.pallas_call(
        functools.partial(pipeline_kernel, n_stage, n_data, n_chunk, 1.0 / (n_data * n_row)),
        out_shape=(out((n_row, width), BF16), out((n_row, ffn), BF16), out((n_row, ffn), F32),
                   out((n_row, ffn), BF16), out((n_row, width), BF16), out((width, ffn), F32), out((ffn, width), F32), out((8, DT), F32)),
        in_specs=[hbm] * 4,
        out_specs=(hbm,) * 7 + (pl.BlockSpec(memory_space=pltpu.VMEM),),
        scratch_shapes=[
            pltpu.VMEM((width, half), BF16), pltpu.VMEM((half, width), BF16),
            pltpu.VMEM((RING, width, CT), BF16), pltpu.VMEM((ROWS, ffn), BF16),
            pltpu.VMEM((5, ROWS, CT), F32), pltpu.VMEM((2, ROWS, width), BF16),
            pltpu.VMEM((2, ROWS, width), BF16), pltpu.VMEM((16, DT), F32),
            pltpu.VMEM((3, 8, DT), F32),
            dma((NSTEP,)), dma((NSTEP,)), dma((RING,)), dma((5,)), dma, dma((2,)), dma((2,)),
            dma((n_chunk,)), dma((n_chunk,)), dma, dma, dma((2,)), dma((2,)), dma, dma((2,)), dma((3,)),
        ],
        compiler_params=pltpu.CompilerParams(collective_id=0, has_side_effects=True, vmem_limit_bytes=67043328),
        cost_estimate=pl.CostEstimate(flops=flops, bytes_accessed=1 << 30, transcendentals=n_row * ffn),
        name='pipeline',
    )(x, y, w1, w2)


def grad_kernel(up, sc, held, lo, hi, part, *rest):
    got, o = rest if len(rest) == 2 else (None, rest[0])
    n = hi.shape[0]

    def product(rows_, tile):
        return dot(held[rows_, :], tile[...], TN) if up else dot(tile[...], held[rows_, :], TN)

    def finish(v):
        o[...] = v if got is None else v + got[...]

    @pl.when(pl.program_id(0) < sc[1])
    def _():
        finish(product(pl.ds(n, n), hi) + part[...])

    @pl.when(pl.program_id(0) >= sc[1])
    def _():
        finish(product(pl.ds(0, n), lo) + product(pl.ds(n, n), hi))


def weight_grad(up, held, streamed, part, side, n_done, got=None):
    n_row, width = held.shape
    half = width // 2
    n_tok = n_row // 2
    ffn = streamed.shape[1]
    shape = (half, DT) if up else (DT, half)

    def at(i, j):
        return (j, i) if up else (i, j)

    specs = [
        pl.BlockSpec((n_row, half), lambda b, sc: (0, sc[0])),
        pl.BlockSpec((n_tok, DT), lambda b, sc: (0, jnp.maximum(b, jnp.minimum(sc[1], N_BLOCK - 1)))),
        pl.BlockSpec((n_tok, DT), lambda b, sc: (1, b)),
        pl.BlockSpec(shape, lambda b, sc: at(jnp.minimum(b, jnp.maximum(sc[1] - 1, 0)), sc[0])),
    ]
    args = [held, streamed, streamed, part]
    if got is not None:
        specs.append(pl.BlockSpec(shape, lambda b, sc: at(b, 0)))
        args.append(got)
    return pl.pallas_call(
        functools.partial(grad_kernel, up),
        out_shape=jax.ShapeDtypeStruct((half, ffn) if up else (ffn, half), F32),
        grid_spec=pltpu.PrefetchScalarGridSpec(
            num_scalar_prefetch=1, grid=(ffn // DT,), in_specs=specs,
            out_specs=pl.BlockSpec(shape, lambda b, sc: at(b, 0))),
        compiler_params=pltpu.CompilerParams(dimension_semantics=('arbitrary',), vmem_limit_bytes=60 * 2**20),
        cost_estimate=pl.CostEstimate(flops=2 * n_row * half * ffn, bytes_accessed=2 * n_row * ffn + 8 * half * ffn, transcendentals=0),
        name='grad_up' if up else 'grad_down',
    )(jnp.stack([side, n_done]).astype(jnp.int32), *args)


def solution(mesh):
    n_stage = mesh.shape['stage']
    n_data = mesh.shape['data']

    def per_device(inputs, targets, w_up, w_down):
        n_micro, n_tok, width = inputs.shape
        n_row = n_micro * n_tok
        x = inputs.reshape(n_row, width)
        y = targets.reshape(n_row, width)
        hs, gs, _, qs, es, up_part, down_part, loss = run_pipeline(n_stage, n_data, x, y, w_up, w_down)
        n_down, n_up, _, _ = early_plan(lax.axis_index('stage'))
        mine = lax.axis_index('data')
        other = n_data - 1 - mine
        swap = [(0, 1), (1, 0)]

        def grad(up, side, got=None):
            if up:
                return weight_grad(True, hs, qs, up_part, side, n_up, got)
            return weight_grad(False, es, gs, down_part, side, n_down, got)

        up_other = lax.ppermute(grad(True, other), 'data', swap)
        down_other = lax.ppermute(grad(False, other), 'data', swap)
        g_up = grad(True, mine, up_other)
        g_down = grad(False, mine, down_other)
        loss_total = jnp.sum(loss) * (0.5 / (n_data * n_row))
        return loss_total, g_up[None], g_down[None]

    return jax.shard_map(per_device, mesh=mesh, in_specs=(P('data', None, None), P('data', None, None), P('stage', None, None), P('stage', None, None)), out_specs=(P(), P('stage', 'data', None), P('stage', None, 'data')), check_vma=False)
```

```python
import functools

import jax
import jax.numpy as jnp
from jax import lax
from jax.experimental import pallas as pl
from jax.experimental.pallas import tpu as pltpu
from jax.sharding import PartitionSpec as P

BF16 = jnp.bfloat16
F32 = jnp.float32
C0 = 0.7978845608028654
C1 = 0.044715
ROWS = 256
CT = 1024
DT = 512
NSTEP = 4
RING = 4
NN = (((1,), (0,)), ((), ()))
NT = (((1,), (1,)), ((), ()))
TN = (((0,), (0,)), ((), ()))


def dot(a, b, dims):
    return lax.dot_general(a, b, dims, preferred_element_type=F32)


N_BLOCK = 16


def early_plan(s):
    n_down = jnp.where(s < 2, N_BLOCK, jnp.where(s == 2, 6, 0))
    n_up = jnp.where(s == 0, 14, jnp.where(s == 1, 4, 0))
    after = jnp.where(s == 2, 12, 8)
    each = jnp.where(s == 0, 60, jnp.where(s == 1, 16, 6))
    return n_down, n_up, after, each


def pipeline_kernel(n_stage, n_data, n_chunk, inv_total,
                    x, y, w1, w2,
                    hs, gs, ds, qs, es, up_part, down_part, loss_out,
                    w1r, w2r, ring, gq, dbuf, inb, out, loss_acc, lbuf,
                    w1_sem, w2_sem, ring_sem, d_sem, gq_sem, in_sem, o_send,
                    h_recv, e_recv, y_sem, st_sem, l_send, l_recv, held_sem, tile_sem, part_sem):
    s = lax.axis_index('stage')
    peer = n_data - 1 - lax.axis_index('data')
    first = s == 0
    last = s == n_stage - 1
    half = w1r.shape[1]
    n_slot = 2 * n_chunk
    warm = jnp.where(first, n_chunk, jnp.where(last, 1, 12 - 4 * s))

    def order(k):
        j = jnp.maximum(k - warm, 0)
        left = n_chunk - warm
        early = k < warm
        mixed = j < 2 * left
        odd = lax.rem(j, 2) == 1
        is_f = early | (mixed & odd)
        idx = jnp.where(early, k, jnp.where(mixed, jnp.where(odd, warm + j // 2, j // 2), j - left))
        return is_f, idx

    def rows(i):
        return pl.ds(pl.multiple_of(i * ROWS, ROWS), ROWS)

    def cols(j, size, base=0):
        if isinstance(j, int):
            return pl.ds(base + j * size, size)
        return pl.ds(pl.multiple_of(base + j * size, size), size)

    def copy(src, dst, sem):
        return pltpu.make_async_copy(src, dst, sem)

    def start_f1(j):
        copy(w1.at[0, :, cols(j, CT, half)], ring.at[j], ring_sem.at[j]).start()

    def start_f2(j):
        for i in range(2):
            copy(w2.at[0, pl.ds(half + i * 2048, 2048), cols(j, DT)], ring.at[j, :, pl.ds(i * DT, DT)], ring_sem.at[j]).start()

    def start_b1(j):
        for i in range(2):
            copy(w2.at[0, cols(j, CT, half), pl.ds(i * CT, CT)], ring.at[j, pl.ds(i * CT, CT)], ring_sem.at[j]).start()

    def start_b2(j):
        for i in range(4):
            copy(w1.at[0, cols(j, DT), pl.ds(half + i * CT, CT)], ring.at[j, pl.ds(i * DT, DT)], ring_sem.at[j]).start()

    def start_slot(k, j):
        is_f, _ = order(k)

        @pl.when((k < n_slot) & is_f)
        def _():
            start_f1(j)

        @pl.when((k < n_slot) & jnp.logical_not(is_f))
        def _():
            start_b1(j)

    def wait_ring(r):
        copy(ring.at[r], ring.at[r], ring_sem.at[r]).wait()

    def d_cols(j, b):
        return cols(j, CT, b * half)

    def d_out_slot(j, b):
        return 2 + lax.rem(j, 3) if b else lax.rem(j, 2)

    def d_in_slot(j, b):
        return 3 * b + lax.rem(j, 2)

    def start_d_in(i, j):
        for b in range(2):
            copy(ds.at[rows(i), d_cols(j, b)], dbuf.at[d_in_slot(j, b)], d_sem.at[d_in_slot(j, b)]).start()

    def start_d_out(i, j, b):
        copy(dbuf.at[d_out_slot(j, b)], ds.at[rows(i), d_cols(j, b)], d_sem.at[d_out_slot(j, b)]).start()

    def wait_d(q):
        copy(dbuf.at[q], dbuf.at[q], d_sem.at[q]).wait()

    def needs_copy(k):
        is_f, _ = order(k)
        return is_f | jnp.logical_not(last)

    def ahead(k):
        is_f, _ = order(k)
        return is_f & (first | (k >= warm)) & (k < n_slot)

    def load_in(k):
        is_f, i = order(k)
        b = lax.rem(k, 2)

        @pl.when(is_f & first)
        def _():
            copy(x.at[rows(i)], inb.at[b], in_sem.at[b]).start()

        @pl.when(is_f & jnp.logical_not(first))
        def _():
            copy(hs.at[rows(i)], hs.at[rows(i)], h_recv.at[i]).wait()
            copy(hs.at[rows(i)], inb.at[b], in_sem.at[b]).start()

        @pl.when(jnp.logical_not(is_f) & jnp.logical_not(last))
        def _():
            copy(es.at[rows(i)], es.at[rows(i)], e_recv.at[i]).wait()
            copy(es.at[rows(i)], inb.at[b], in_sem.at[b]).start()

    def before_next(k):
        is_f, i = order(k + 1)

        @pl.when(ahead(k + 1))
        def _():
            load_in(k + 1)

        @pl.when((k + 1 < n_slot) & jnp.logical_not(is_f))
        def _():
            start_d_in(i, 0)

    def next_stage(k, i, j):
        o = lax.rem(k, 2)
        return pltpu.make_async_remote_copy(
            src_ref=out.at[o, :, cols(j, DT)], dst_ref=hs.at[rows(i), cols(j, DT)],
            send_sem=o_send.at[o], recv_sem=h_recv.at[i],
            device_id={'stage': s + 1}, device_id_type=pl.DeviceIdType.MESH)

    def prev_stage(k, i, j):
        o = lax.rem(k, 2)
        return pltpu.make_async_remote_copy(
            src_ref=out.at[o, :, cols(j, DT)], dst_ref=es.at[rows(i), cols(j, DT)],
            send_sem=o_send.at[o], recv_sem=e_recv.at[i],
            device_id={'stage': s - 1}, device_id_type=pl.DeviceIdType.MESH)

    def sent(k):
        is_f, _ = order(k)
        return (is_f & jnp.logical_not(last)) | (jnp.logical_not(is_f) & jnp.logical_not(first))

    def wait_sent(k):
        @pl.when((k >= 0) & sent(jnp.maximum(k, 0)))
        def _():
            o = lax.rem(k, 2)
            copy(out.at[o], out.at[o], o_send.at[o]).wait()

    def gelu_tile(q, c, lo, hi):
        for r in range(0, ROWS, 16):
            for z in range(lo, hi, 256):
                u = dbuf[q, pl.ds(r, 16), pl.ds(z, 256)]
                u2 = u * u
                h = 0.5 * jnp.tanh(u * (C0 + (C0 * C1) * u2)) + 0.5
                g = u * h
                gq[pl.ds(r, 16), pl.ds(pl.multiple_of(c + z, 256), 256)] = g.astype(BF16)
                dbuf[q, pl.ds(r, 16), pl.ds(z, 256)] = h + (g * (1.0 - h)) * (2.0 * C0 + (6.0 * C0 * C1) * u2)

    def g_out(i, j, b):
        copy(gq.at[:, d_cols(j, b)], gs.at[rows(i), d_cols(j, b)], gq_sem).start()

    def forward(k, i):
        p = lax.rem(k, 2)
        o = lax.rem(k, 2)

        def step1(j, carry):
            @pl.when(j == 0)
            def _():
                start_f1(2)
                start_f1(3)

            @pl.when(j >= 1)
            def _():
                start_f2(j - 1)

            @pl.when(j >= 2)
            def _():
                wait_d(lax.rem(j, 2))

            @pl.when(j >= 3)
            def _():
                wait_d(2)

            @pl.when(k == 0)
            def _():
                copy(w1r.at[:, cols(j, CT)], w1r.at[:, cols(j, CT)], w1_sem.at[j]).wait()

            wait_ring(j)
            jp = jnp.maximum(j - 1, 0)
            res, stm, old = d_out_slot(j, 0), d_out_slot(j, 1), 2 + lax.rem(j + 2, 3)
            old_at, res_at = half + jp * CT, j * CT
            dbuf[res, :, pl.ds(0, DT)] = dot(inb[p], w1r[:, cols(2 * j, DT)], NN)
            gelu_tile(old, old_at, 0, 768)
            dbuf[res, :, pl.ds(DT, DT)] = dot(inb[p], w1r[:, cols(2 * j + 1, DT)], NN)
            gelu_tile(old, old_at, 768, CT)
            gelu_tile(res, res_at, 0, 512)
            dbuf[stm, :, pl.ds(0, DT)] = dot(inb[p], ring[j, :, pl.ds(0, DT)], NN)
            gelu_tile(res, res_at, 512, CT)
            dbuf[stm, :, pl.ds(DT, DT)] = dot(inb[p], ring[j, :, pl.ds(DT, DT)], NN)

            @pl.when(j >= 1)
            def _():
                g_out(i, j - 1, 1)
                start_d_out(i, j - 1, 1)

            g_out(i, j, 0)
            start_d_out(i, j, 0)
            return carry

        lax.fori_loop(0, NSTEP, step1, 0)

        @pl.when(last)
        def _():
            copy(inb.at[1 - p], inb.at[1 - p], y_sem).wait()

        wait_sent(k - 2)
        for jj in range(2):
            if jj == 0:
                start_f2(3)
                wait_d(3)
            else:
                start_slot(k + 1, 0)
                start_slot(k + 1, 1)
                for q in (0, 1, 4):
                    wait_d(q)
                before_next(k)

            @pl.when(k == 0)
            def _():
                for j in (2 * jj, 2 * jj + 1):
                    copy(w2r.at[:, cols(j, DT)], w2r.at[:, cols(j, DT)], w2_sem.at[j]).wait()

            for j in (2 * jj, 2 * jj + 1):
                wait_ring(j)
            for j in (2 * jj, 2 * jj + 1):
                v = dot(gq[:, pl.ds(0, half)], w2r[:, cols(j, DT)], NN)
                if j == 0:
                    dbuf[3, :, pl.ds(0, DT)] = v
                    gelu_tile(2, half + 3 * CT, 0, CT)
                    v = dbuf[3, :, pl.ds(0, DT)]
                v = v + dot(gq[:, pl.ds(half, 2048)], ring[j, :, pl.ds(0, DT)], NN)
                v = v + dot(gq[:, pl.ds(half + 2048, 2048)], ring[j, :, pl.ds(DT, DT)], NN)
                out[o, :, cols(j, DT)] = (inb[p, :, cols(j, DT)].astype(F32) + v).astype(BF16)
            if jj == 0:
                g_out(i, 3, 1)
                start_d_out(i, 3, 1)

            @pl.when(jnp.logical_not(last))
            def _():
                for j in (2 * jj, 2 * jj + 1):
                    next_stage(k, i, j).start()

            @pl.when(last)
            def _():
                for j in (2 * jj, 2 * jj + 1):
                    for r in range(0, ROWS, 16):
                        diff = out[o, pl.ds(r, 16), cols(j, DT)].astype(F32) - inb[1 - p, pl.ds(r, 16), cols(j, DT)].astype(F32)
                        loss_acc[...] += diff * diff
                        inb[1 - p, pl.ds(r, 16), cols(j, DT)] = (diff * inv_total).astype(BF16)

        wait_d(2)

    def backward(k, i):
        p = lax.rem(k, 2)
        o = lax.rem(k, 2)

        def step1(j, carry):
            @pl.when(j == 0)
            def _():
                start_b1(2)
                start_b1(3)

            @pl.when((j >= 1) & jnp.logical_not(first))
            def _():
                start_b2(j - 1)

            @pl.when((j >= 1) & (j < 3) & first)
            def _():
                start_slot(k + 1, j - 1)

            @pl.when(j < NSTEP - 1)
            def _():
                start_d_in(i, j + 1)

            @pl.when((j == NSTEP - 1) & first)
            def _():
                before_next(k)

            wait_d(d_in_slot(j, 0))
            wait_d(d_in_slot(j, 1))
            wait_ring(j)
            pa = dot(inb[p], w2r[cols(j, CT), :], NT).astype(BF16).astype(F32)
            gq[:, d_cols(j, 0)] = (pa * dbuf[d_in_slot(j, 0)]).astype(BF16)
            pb = dot(inb[p, :, pl.ds(0, CT)], ring[j, pl.ds(0, CT)], NT)
            pb = pb + dot(inb[p, :, pl.ds(CT, CT)], ring[j, pl.ds(CT, CT)], NT)
            pb = pb.astype(BF16).astype(F32)
            gq[:, d_cols(j, 1)] = (pb * dbuf[d_in_slot(j, 1)]).astype(BF16)
            for b in range(2):
                copy(gq.at[:, d_cols(j, b)], qs.at[rows(i), d_cols(j, b)], gq_sem).start()
            return carry

        lax.fori_loop(0, NSTEP, step1, 0)
        wait_sent(k - 2)

        @pl.when(jnp.logical_not(first))
        def _():
            def step2(jj, carry):
                @pl.when(jj == 0)
                def _():
                    start_b2(3)

                @pl.when(jj == 1)
                def _():
                    start_slot(k + 1, 0)
                    start_slot(k + 1, 1)
                    before_next(k)

                for z in range(2):
                    wait_ring(2 * jj + z)
                for z in range(2):
                    j = 2 * jj + z
                    v = dot(gq[:, pl.ds(0, half)], w1r[cols(j, DT), :], NT)
                    for c in range(4):
                        v = v + dot(gq[:, pl.ds(half + c * CT, CT)], ring[j, pl.ds(c * DT, DT)], NT)
                    out[o, :, cols(j, DT)] = (inb[p, :, cols(j, DT)].astype(F32) + v).astype(BF16)
                for z in range(2):
                    prev_stage(k, i, 2 * jj + z).start()
                return carry

            lax.fori_loop(0, 2, step2, 0)

    def early_units(i):
        n_down, n_up, after, each = early_plan(s)
        n_unit = 2 * (n_down + n_up)
        lo = jnp.clip((i - after) * each, 0, n_unit)
        return lo, jnp.where(i >= after, jnp.clip((i - after + 1) * each, 0, n_unit), lo)

    def early(i):
        lo, hi = early_units(i)
        n_tok = ring.shape[1]
        n_down, n_up, _, _ = early_plan(s)

        def place(u):
            down = u < 2 * n_down
            v = jnp.where(down, u, u - 2 * n_down)
            n = jnp.maximum(jnp.where(down, n_down, n_up), 1)
            side = jnp.where(v >= n, 1, 0)
            return down, side, v - n * side


        def tile(u, start):
            dst = ring.at[3, :, pl.ds(pl.multiple_of(lax.rem(u, 2) * DT, DT), DT)]
            sem = tile_sem.at[lax.rem(u, 2)]
            if not start:
                copy(dst, dst, sem).wait()
                return
            down, _, b = place(u)

            @pl.when(down)
            def _():
                copy(gs.at[pl.ds(0, n_tok), cols(b, DT)], dst, sem).start()

            @pl.when(jnp.logical_not(down))
            def _():
                copy(qs.at[pl.ds(0, n_tok), cols(b, DT)], dst, sem).start()

        def part_slot(t):
            z = lax.rem(t, 3)
            return jnp.where(z == 2, 4, z + 1)

        def wait_part(t):
            q = part_slot(t)
            copy(dbuf.at[q], dbuf.at[q], part_sem.at[lax.rem(t, 3)]).wait()

        def unit(u, carry):
            down, hf, b = place(u)
            c0 = lax.rem(u, 2) * DT

            @pl.when((u == lo) | (b == 0))
            def _():
                @pl.when(down)
                def _():
                    copy(es.at[pl.ds(0, n_tok), cols(hf, CT)], ring.at[2], held_sem).start()

                @pl.when(jnp.logical_not(down))
                def _():
                    copy(hs.at[pl.ds(0, n_tok), cols(hf, CT)], ring.at[2], held_sem).start()

            @pl.when(u == lo)
            def _():
                tile(u, True)

            @pl.when(u + 1 < hi)
            def _():
                tile(u + 1, True)

            @pl.when((u == lo) | (b == 0))
            def _():
                copy(ring.at[2], ring.at[2], held_sem).wait()

            tile(u, False)
            for z in range(2):
                t = 2 * (u - lo) + z
                q = part_slot(t)

                @pl.when(t >= 3)
                def _():
                    wait_part(t)

                @pl.when(down)
                def _():
                    dbuf[q] = dot(ring[3, :, pl.ds(pl.multiple_of(c0 + z * ROWS, ROWS), ROWS)], ring[2], TN)
                    copy(dbuf.at[q], down_part.at[cols(2 * b + z, ROWS), cols(hf, CT)], part_sem.at[lax.rem(t, 3)]).start()

                @pl.when(jnp.logical_not(down))
                def _():
                    for a in range(2):
                        r = 2 * z + a
                        dbuf[q, :, pl.ds(a * DT, DT)] = dot(ring[2, :, pl.ds(r * ROWS, ROWS)], ring[3, :, pl.ds(pl.multiple_of(c0, DT), DT)], TN)
                    for a in range(2):
                        r = 2 * z + a
                        copy(dbuf.at[q, :, pl.ds(a * DT, DT)], up_part.at[cols(4 * hf + r, ROWS), cols(b, DT)], part_sem.at[lax.rem(t, 3)]).start()
            return carry

        lax.fori_loop(lo, hi, unit, 0)

        @pl.when(hi > lo)
        def _():
            wait_part(2 * (hi - lo) - 1)
            wait_part(2 * (hi - lo) - 2)

        @pl.when(hi > lo + 1)
        def _():
            wait_part(2 * (hi - lo) - 3)

    barrier = pltpu.get_barrier_semaphore()

    def hello(**to):
        pl.semaphore_signal(barrier, inc=1, device_id=to, device_id_type=pl.DeviceIdType.MESH)

    @pl.when(jnp.logical_not(first))
    def _():
        hello(stage=s - 1)

    @pl.when(jnp.logical_not(last))
    def _():
        hello(stage=s + 1)

    @pl.when(last)
    def _():
        hello(data=peer)

    @pl.when(first)
    def _():
        load_in(0)

    start_f1(0)
    for j in range(NSTEP):
        copy(w1.at[0, :, pl.ds(j * CT, CT)], w1r.at[:, pl.ds(j * CT, CT)], w1_sem.at[j]).start()
        if j == 0:
            start_f1(1)
    for j in range(NSTEP):
        copy(w2.at[0, pl.ds(0, half), pl.ds(j * DT, DT)], w2r.at[:, pl.ds(j * DT, DT)], w2_sem.at[j]).start()
    loss_acc[...] = jnp.zeros_like(loss_acc)

    @pl.when(first)
    def _():
        pl.semaphore_wait(barrier, 1)

    @pl.when(jnp.logical_not(first))
    def _():
        pl.semaphore_wait(barrier, 2)

    def slot(k, carry):
        is_f, i = order(k)
        p = lax.rem(k, 2)

        @pl.when(k > 0)
        def _():
            copy(gq, gq, gq_sem).wait()

        @pl.when(jnp.logical_not(ahead(k)))
        def _():
            load_in(k)

        @pl.when(needs_copy(k))
        def _():
            copy(inb.at[p], inb.at[p], in_sem.at[p]).wait()

        @pl.when(is_f & first)
        def _():
            copy(inb.at[p], hs.at[rows(i)], st_sem).start()

        @pl.when(jnp.logical_not(is_f) & last)
        def _():
            copy(inb.at[p], es.at[rows(i)], st_sem).start()

        @pl.when(is_f & last)
        def _():
            copy(y.at[rows(i)], inb.at[1 - p], y_sem).start()

        @pl.when(is_f)
        def _():
            forward(k, i)

        @pl.when(jnp.logical_not(is_f))
        def _():
            backward(k, i)

        @pl.when((is_f & first) | (jnp.logical_not(is_f) & last))
        def _():
            copy(inb.at[p], inb.at[p], st_sem).wait()

        @pl.when(jnp.logical_not(is_f))
        def _():
            early(i)

        return carry

    lax.fori_loop(0, n_slot, slot, 0)
    copy(gq, gq, gq_sem).wait()
    for k in range(n_slot - 2, n_slot):
        wait_sent(jnp.int32(k))

    def to_peer():
        return pltpu.make_async_remote_copy(
            src_ref=lbuf.at[0], dst_ref=lbuf.at[1], send_sem=l_send.at[0], recv_sem=l_recv.at[0],
            device_id={'data': peer}, device_id_type=pl.DeviceIdType.MESH)

    def to_prev():
        return pltpu.make_async_remote_copy(
            src_ref=lbuf.at[2], dst_ref=lbuf.at[2], send_sem=l_send.at[1], recv_sem=l_recv.at[1],
            device_id={'stage': s - 1}, device_id_type=pl.DeviceIdType.MESH)

    @pl.when(last)
    def _():
        lbuf[0] = loss_acc[pl.ds(0, 8), :] + loss_acc[pl.ds(8, 8), :]
        rdma = to_peer()
        rdma.start()
        rdma.wait()
        lbuf[2] = lbuf[0] + lbuf[1]

    @pl.when(jnp.logical_not(last))
    def _():
        copy(lbuf.at[2], lbuf.at[2], l_recv.at[1]).wait()

    loss_out[...] = lbuf[2]

    @pl.when(jnp.logical_not(first))
    def _():
        to_prev().start()
        copy(lbuf.at[2], lbuf.at[2], l_send.at[1]).wait()


def run_pipeline(n_stage, n_data, x, y, w1, w2):
    n_row, width = x.shape
    ffn = w1.shape[2]
    n_chunk = n_row // ROWS
    half = ffn // 2
    hbm = pl.BlockSpec(memory_space=pl.ANY)
    out = jax.ShapeDtypeStruct
    dma = pltpu.SemaphoreType.DMA
    flops = 8 * n_row * width * ffn
    return pl.pallas_call(
        functools.partial(pipeline_kernel, n_stage, n_data, n_chunk, 1.0 / (n_data * n_row)),
        out_shape=(out((n_row, width), BF16), out((n_row, ffn), BF16), out((n_row, ffn), F32),
                   out((n_row, ffn), BF16), out((n_row, width), BF16), out((width, ffn), F32), out((ffn, width), F32), out((8, DT), F32)),
        in_specs=[hbm] * 4,
        out_specs=(hbm,) * 7 + (pl.BlockSpec(memory_space=pltpu.VMEM),),
        scratch_shapes=[
            pltpu.VMEM((width, half), BF16), pltpu.VMEM((half, width), BF16),
            pltpu.VMEM((RING, width, CT), BF16), pltpu.VMEM((ROWS, ffn), BF16),
            pltpu.VMEM((5, ROWS, CT), F32), pltpu.VMEM((2, ROWS, width), BF16),
            pltpu.VMEM((2, ROWS, width), BF16), pltpu.VMEM((16, DT), F32),
            pltpu.VMEM((3, 8, DT), F32),
            dma((NSTEP,)), dma((NSTEP,)), dma((RING,)), dma((5,)), dma, dma((2,)), dma((2,)),
            dma((n_chunk,)), dma((n_chunk,)), dma, dma, dma((2,)), dma((2,)), dma, dma((2,)), dma((3,)),
        ],
        compiler_params=pltpu.CompilerParams(collective_id=0, has_side_effects=True, vmem_limit_bytes=67043328),
        cost_estimate=pl.CostEstimate(flops=flops, bytes_accessed=1 << 30, transcendentals=n_row * ffn),
        name='pipeline',
    )(x, y, w1, w2)


def grad_kernel(up, sc, held, lo, hi, part, *rest):
    got, o = rest if len(rest) == 2 else (None, rest[0])
    n = hi.shape[0]

    def product(rows_, tile):
        return dot(held[rows_, :], tile[...], TN) if up else dot(tile[...], held[rows_, :], TN)

    def finish(v):
        o[...] = v if got is None else v + got[...]

    @pl.when(pl.program_id(0) < sc[1])
    def _():
        finish(product(pl.ds(n, n), hi) + part[...])

    @pl.when(pl.program_id(0) >= sc[1])
    def _():
        finish(product(pl.ds(0, n), lo) + product(pl.ds(n, n), hi))


def weight_grad(up, held, streamed, part, side, n_done, got=None):
    n_row, width = held.shape
    half = width // 2
    n_tok = n_row // 2
    ffn = streamed.shape[1]
    shape = (half, DT) if up else (DT, half)

    def at(i, j):
        return (j, i) if up else (i, j)

    specs = [
        pl.BlockSpec((n_row, half), lambda b, sc: (0, sc[0])),
        pl.BlockSpec((n_tok, DT), lambda b, sc: (0, jnp.maximum(b, jnp.minimum(sc[1], N_BLOCK - 1)))),
        pl.BlockSpec((n_tok, DT), lambda b, sc: (1, b)),
        pl.BlockSpec(shape, lambda b, sc: at(jnp.minimum(b, jnp.maximum(sc[1] - 1, 0)), sc[0])),
    ]
    args = [held, streamed, streamed, part]
    if got is not None:
        specs.append(pl.BlockSpec(shape, lambda b, sc: at(b, 0)))
        args.append(got)
    return pl.pallas_call(
        functools.partial(grad_kernel, up),
        out_shape=jax.ShapeDtypeStruct((half, ffn) if up else (ffn, half), F32),
        grid_spec=pltpu.PrefetchScalarGridSpec(
            num_scalar_prefetch=1, grid=(ffn // DT,), in_specs=specs,
            out_specs=pl.BlockSpec(shape, lambda b, sc: at(b, 0))),
        compiler_params=pltpu.CompilerParams(dimension_semantics=('arbitrary',), vmem_limit_bytes=60 * 2**20),
        cost_estimate=pl.CostEstimate(flops=2 * n_row * half * ffn, bytes_accessed=2 * n_row * ffn + 8 * half * ffn, transcendentals=0),
        name='grad_up' if up else 'grad_down',
    )(jnp.stack([side, n_done]).astype(jnp.int32), *args)


def solution(mesh):
    n_stage = mesh.shape['stage']
    n_data = mesh.shape['data']

    def per_device(inputs, targets, w_up, w_down):
        n_micro, n_tok, width = inputs.shape
        n_row = n_micro * n_tok
        x = inputs.reshape(n_row, width)
        y = targets.reshape(n_row, width)
        hs, gs, _, qs, es, up_part, down_part, loss = run_pipeline(n_stage, n_data, x, y, w_up, w_down)
        n_down, n_up, _, _ = early_plan(lax.axis_index('stage'))
        mine = lax.axis_index('data')
        other = n_data - 1 - mine
        swap = [(0, 1), (1, 0)]

        def grad(up, side, got=None):
            if up:
                return weight_grad(True, hs, qs, up_part, side, n_up, got)
            return weight_grad(False, es, gs, down_part, side, n_down, got)

        up_other = lax.ppermute(grad(True, other), 'data', swap)
        down_other = lax.ppermute(grad(False, other), 'data', swap)
        g_up = grad(True, mine, up_other)
        g_down = grad(False, mine, down_other)
        loss_total = jnp.sum(loss) * (0.5 / (n_data * n_row))
        return loss_total, g_up[None], g_down[None]

    return jax.shard_map(per_device, mesh=mesh, in_specs=(P('data', None, None), P('data', None, None), P('stage', None, None), P('stage', None, None)), out_specs=(P(), P('stage', 'data', None), P('stage', None, 'data')), check_vma=False)
```

```python
import functools

import jax
import jax.numpy as jnp
from jax import lax
from jax.experimental import pallas as pl
from jax.experimental.pallas import tpu as pltpu
from jax.sharding import PartitionSpec as P

BF16 = jnp.bfloat16
F32 = jnp.float32
C0 = 0.7978845608028654
C1 = 0.044715
ROWS = 256
CT = 1024
DT = 512
NSTEP = 4
RING = 4
NN = (((1,), (0,)), ((), ()))
NT = (((1,), (1,)), ((), ()))
TN = (((0,), (0,)), ((), ()))


def dot(a, b, dims):
    return lax.dot_general(a, b, dims, preferred_element_type=F32)


N_BLOCK = 16


def early_plan(s):
    n_down = jnp.where(s < 2, N_BLOCK, jnp.where(s == 2, 8, 0))
    n_up = jnp.where(s == 0, 14, jnp.where(s == 1, 2, 0))
    after = jnp.where(s == 2, 12, 8)
    each = jnp.where(s == 0, 60, jnp.where(s == 1, 16, 8))
    return n_down, n_up, after, each


def pipeline_kernel(n_stage, n_data, n_chunk, inv_total,
                    x, y, w1, w2,
                    hs, gs, ds, qs, es, up_part, down_part, loss_out,
                    w1r, w2r, ring, gq, dbuf, inb, out, loss_acc, lbuf,
                    w1_sem, w2_sem, ring_sem, d_sem, gq_sem, in_sem, o_send,
                    h_recv, e_recv, y_sem, st_sem, l_send, l_recv, held_sem, tile_sem, part_sem):
    s = lax.axis_index('stage')
    peer = n_data - 1 - lax.axis_index('data')
    first = s == 0
    last = s == n_stage - 1
    half = w1r.shape[1]
    n_slot = 2 * n_chunk
    warm = jnp.where(first, n_chunk, jnp.where(last, 1, 12 - 4 * s))

    def order(k):
        j = jnp.maximum(k - warm, 0)
        left = n_chunk - warm
        early = k < warm
        mixed = j < 2 * left
        odd = lax.rem(j, 2) == 1
        is_f = early | (mixed & odd)
        idx = jnp.where(early, k, jnp.where(mixed, jnp.where(odd, warm + j // 2, j // 2), j - left))
        return is_f, idx

    def rows(i):
        return pl.ds(pl.multiple_of(i * ROWS, ROWS), ROWS)

    def cols(j, size, base=0):
        if isinstance(j, int):
            return pl.ds(base + j * size, size)
        return pl.ds(pl.multiple_of(base + j * size, size), size)

    def copy(src, dst, sem):
        return pltpu.make_async_copy(src, dst, sem)

    def start_f1(j):
        copy(w1.at[0, :, cols(j, CT, half)], ring.at[j], ring_sem.at[j]).start()

    def start_f2(j):
        for i in range(2):
            copy(w2.at[0, pl.ds(half + i * 2048, 2048), cols(j, DT)], ring.at[j, :, pl.ds(i * DT, DT)], ring_sem.at[j]).start()

    def start_b1(j):
        for i in range(2):
            copy(w2.at[0, cols(j, CT, half), pl.ds(i * CT, CT)], ring.at[j, pl.ds(i * CT, CT)], ring_sem.at[j]).start()

    def start_b2(j):
        for i in range(4):
            copy(w1.at[0, cols(j, DT), pl.ds(half + i * CT, CT)], ring.at[j, pl.ds(i * DT, DT)], ring_sem.at[j]).start()

    def start_slot(k, j):
        is_f, _ = order(k)

        @pl.when((k < n_slot) & is_f)
        def _():
            start_f1(j)

        @pl.when((k < n_slot) & jnp.logical_not(is_f))
        def _():
            start_b1(j)

    def wait_ring(r):
        copy(ring.at[r], ring.at[r], ring_sem.at[r]).wait()

    def d_cols(j, b):
        return cols(j, CT, b * half)

    def d_out_slot(j, b):
        return 2 + lax.rem(j, 3) if b else lax.rem(j, 2)

    def d_in_slot(j, b):
        return 3 * b + lax.rem(j, 2)

    def start_d_in(i, j):
        for b in range(2):
            copy(ds.at[rows(i), d_cols(j, b)], dbuf.at[d_in_slot(j, b)], d_sem.at[d_in_slot(j, b)]).start()

    def start_d_out(i, j, b):
        copy(dbuf.at[d_out_slot(j, b)], ds.at[rows(i), d_cols(j, b)], d_sem.at[d_out_slot(j, b)]).start()

    def wait_d(q):
        copy(dbuf.at[q], dbuf.at[q], d_sem.at[q]).wait()

    def needs_copy(k):
        is_f, _ = order(k)
        return is_f | jnp.logical_not(last)

    def ahead(k):
        is_f, _ = order(k)
        return is_f & (first | (k >= warm)) & (k < n_slot)

    def load_in(k):
        is_f, i = order(k)
        b = lax.rem(k, 2)

        @pl.when(is_f & first)
        def _():
            copy(x.at[rows(i)], inb.at[b], in_sem.at[b]).start()

        @pl.when(is_f & jnp.logical_not(first))
        def _():
            copy(hs.at[rows(i)], hs.at[rows(i)], h_recv.at[i]).wait()
            copy(hs.at[rows(i)], inb.at[b], in_sem.at[b]).start()

        @pl.when(jnp.logical_not(is_f) & jnp.logical_not(last))
        def _():
            copy(es.at[rows(i)], es.at[rows(i)], e_recv.at[i]).wait()
            copy(es.at[rows(i)], inb.at[b], in_sem.at[b]).start()

    def before_next(k):
        is_f, i = order(k + 1)

        @pl.when(ahead(k + 1))
        def _():
            load_in(k + 1)

        @pl.when((k + 1 < n_slot) & jnp.logical_not(is_f))
        def _():
            start_d_in(i, 0)

    def next_stage(k, i, j):
        o = lax.rem(k, 2)
        return pltpu.make_async_remote_copy(
            src_ref=out.at[o, :, cols(j, DT)], dst_ref=hs.at[rows(i), cols(j, DT)],
            send_sem=o_send.at[o], recv_sem=h_recv.at[i],
            device_id={'stage': s + 1}, device_id_type=pl.DeviceIdType.MESH)

    def prev_stage(k, i, j):
        o = lax.rem(k, 2)
        return pltpu.make_async_remote_copy(
            src_ref=out.at[o, :, cols(j, DT)], dst_ref=es.at[rows(i), cols(j, DT)],
            send_sem=o_send.at[o], recv_sem=e_recv.at[i],
            device_id={'stage': s - 1}, device_id_type=pl.DeviceIdType.MESH)

    def sent(k):
        is_f, _ = order(k)
        return (is_f & jnp.logical_not(last)) | (jnp.logical_not(is_f) & jnp.logical_not(first))

    def wait_sent(k):
        @pl.when((k >= 0) & sent(jnp.maximum(k, 0)))
        def _():
            o = lax.rem(k, 2)
            copy(out.at[o], out.at[o], o_send.at[o]).wait()

    def gelu_tile(q, c, lo, hi):
        for r in range(0, ROWS, 16):
            for z in range(lo, hi, 256):
                u = dbuf[q, pl.ds(r, 16), pl.ds(z, 256)]
                u2 = u * u
                h = 0.5 * jnp.tanh(u * (C0 + (C0 * C1) * u2)) + 0.5
                g = u * h
                gq[pl.ds(r, 16), pl.ds(pl.multiple_of(c + z, 256), 256)] = g.astype(BF16)
                dbuf[q, pl.ds(r, 16), pl.ds(z, 256)] = h + (g * (1.0 - h)) * (2.0 * C0 + (6.0 * C0 * C1) * u2)

    def g_out(i, j, b):
        copy(gq.at[:, d_cols(j, b)], gs.at[rows(i), d_cols(j, b)], gq_sem).start()

    def forward(k, i):
        p = lax.rem(k, 2)
        o = lax.rem(k, 2)

        def step1(j, carry):
            @pl.when(j == 0)
            def _():
                start_f1(2)
                start_f1(3)

            @pl.when(j >= 1)
            def _():
                start_f2(j - 1)

            @pl.when(j >= 2)
            def _():
                wait_d(lax.rem(j, 2))

            @pl.when(j >= 3)
            def _():
                wait_d(2)

            @pl.when(k == 0)
            def _():
                copy(w1r.at[:, cols(j, CT)], w1r.at[:, cols(j, CT)], w1_sem.at[j]).wait()

            wait_ring(j)
            jp = jnp.maximum(j - 1, 0)
            res, stm, old = d_out_slot(j, 0), d_out_slot(j, 1), 2 + lax.rem(j + 2, 3)
            old_at, res_at = half + jp * CT, j * CT
            dbuf[res, :, pl.ds(0, DT)] = dot(inb[p], w1r[:, cols(2 * j, DT)], NN)
            gelu_tile(old, old_at, 0, 768)
            dbuf[res, :, pl.ds(DT, DT)] = dot(inb[p], w1r[:, cols(2 * j + 1, DT)], NN)
            gelu_tile(old, old_at, 768, CT)
            gelu_tile(res, res_at, 0, 512)
            dbuf[stm, :, pl.ds(0, DT)] = dot(inb[p], ring[j, :, pl.ds(0, DT)], NN)
            gelu_tile(res, res_at, 512, CT)
            dbuf[stm, :, pl.ds(DT, DT)] = dot(inb[p], ring[j, :, pl.ds(DT, DT)], NN)

            @pl.when(j >= 1)
            def _():
                g_out(i, j - 1, 1)
                start_d_out(i, j - 1, 1)

            g_out(i, j, 0)
            start_d_out(i, j, 0)
            return carry

        lax.fori_loop(0, NSTEP, step1, 0)

        @pl.when(last)
        def _():
            copy(inb.at[1 - p], inb.at[1 - p], y_sem).wait()

        wait_sent(k - 2)
        for jj in range(2):
            if jj == 0:
                start_f2(3)
                wait_d(3)
            else:
                start_slot(k + 1, 0)
                start_slot(k + 1, 1)
                for q in (0, 1, 4):
                    wait_d(q)
                before_next(k)

            @pl.when(k == 0)
            def _():
                for j in (2 * jj, 2 * jj + 1):
                    copy(w2r.at[:, cols(j, DT)], w2r.at[:, cols(j, DT)], w2_sem.at[j]).wait()

            for j in (2 * jj, 2 * jj + 1):
                wait_ring(j)
            for j in (2 * jj, 2 * jj + 1):
                v = dot(gq[:, pl.ds(0, half)], w2r[:, cols(j, DT)], NN)
                if j == 0:
                    dbuf[3, :, pl.ds(0, DT)] = v
                    gelu_tile(2, half + 3 * CT, 0, CT)
                    v = dbuf[3, :, pl.ds(0, DT)]
                v = v + dot(gq[:, pl.ds(half, 2048)], ring[j, :, pl.ds(0, DT)], NN)
                v = v + dot(gq[:, pl.ds(half + 2048, 2048)], ring[j, :, pl.ds(DT, DT)], NN)
                out[o, :, cols(j, DT)] = (inb[p, :, cols(j, DT)].astype(F32) + v).astype(BF16)
            if jj == 0:
                g_out(i, 3, 1)
                start_d_out(i, 3, 1)

            @pl.when(jnp.logical_not(last))
            def _():
                for j in (2 * jj, 2 * jj + 1):
                    next_stage(k, i, j).start()

            @pl.when(last)
            def _():
                def pieces(c, carry):
                    for j in (2 * jj, 2 * jj + 1):
                        for z in range(0, 32, 16):
                            r = pl.ds(pl.multiple_of(c * 32 + z, 16), 16)
                            diff = out[o, r, cols(j, DT)].astype(F32) - inb[1 - p, r, cols(j, DT)].astype(F32)
                            loss_acc[...] += diff * diff
                            inb[1 - p, r, cols(j, DT)] = (diff * inv_total).astype(BF16)
                    return carry

                lax.fori_loop(0, ROWS // 32, pieces, 0)

        wait_d(2)

    def backward(k, i):
        p = lax.rem(k, 2)
        o = lax.rem(k, 2)

        def step1(j, carry):
            @pl.when(j == 0)
            def _():
                start_b1(2)
                start_b1(3)

            @pl.when((j >= 1) & jnp.logical_not(first))
            def _():
                start_b2(j - 1)

            @pl.when((j >= 1) & (j < 3) & first)
            def _():
                start_slot(k + 1, j - 1)

            @pl.when(j < NSTEP - 1)
            def _():
                start_d_in(i, j + 1)

            @pl.when((j == NSTEP - 1) & first)
            def _():
                before_next(k)

            wait_d(d_in_slot(j, 0))
            wait_d(d_in_slot(j, 1))
            wait_ring(j)
            for z in range(2):
                pa = dot(inb[p], w2r[cols(2 * j + z, DT), :], NT).astype(BF16).astype(F32)
                gq[:, cols(2 * j + z, DT)] = (pa * dbuf[d_in_slot(j, 0), :, pl.ds(z * DT, DT)]).astype(BF16)
            for z in range(2):
                pb = dot(inb[p, :, pl.ds(0, CT)], ring[j, pl.ds(z * DT, DT)], NT)
                pb = pb + dot(inb[p, :, pl.ds(CT, CT)], ring[j, pl.ds(CT + z * DT, DT)], NT)
                pb = pb.astype(BF16).astype(F32)
                gq[:, cols(2 * j + z, DT, half)] = (pb * dbuf[d_in_slot(j, 1), :, pl.ds(z * DT, DT)]).astype(BF16)
            for b in range(2):
                copy(gq.at[:, d_cols(j, b)], qs.at[rows(i), d_cols(j, b)], gq_sem).start()
            return carry

        lax.fori_loop(0, NSTEP, step1, 0)
        wait_sent(k - 2)

        @pl.when(jnp.logical_not(first))
        def _():
            def step2(jj, carry):
                @pl.when(jj == 0)
                def _():
                    start_b2(3)

                @pl.when(jj == 1)
                def _():
                    start_slot(k + 1, 0)
                    start_slot(k + 1, 1)
                    before_next(k)

                for z in range(2):
                    wait_ring(2 * jj + z)
                for z in range(2):
                    j = 2 * jj + z
                    v = dot(gq[:, pl.ds(0, half)], w1r[cols(j, DT), :], NT)
                    for c in range(4):
                        v = v + dot(gq[:, pl.ds(half + c * CT, CT)], ring[j, pl.ds(c * DT, DT)], NT)
                    out[o, :, cols(j, DT)] = (inb[p, :, cols(j, DT)].astype(F32) + v).astype(BF16)
                for z in range(2):
                    prev_stage(k, i, 2 * jj + z).start()
                return carry

            lax.fori_loop(0, 2, step2, 0)

    def early_units(i):
        n_down, n_up, after, each = early_plan(s)
        n_unit = 2 * (n_down + n_up)
        lo = jnp.clip((i - after) * each, 0, n_unit)
        return lo, jnp.where(i >= after, jnp.clip((i - after + 1) * each, 0, n_unit), lo)

    def early(i):
        lo, hi = early_units(i)
        n_tok = ring.shape[1]
        n_down, n_up, _, _ = early_plan(s)

        def place(u):
            down = u < 2 * n_down
            v = jnp.where(down, u, u - 2 * n_down)
            n = jnp.maximum(jnp.where(down, n_down, n_up), 1)
            side = jnp.where(v >= n, 1, 0)
            return down, side, v - n * side


        def tile(u, start):
            dst = ring.at[3, :, pl.ds(pl.multiple_of(lax.rem(u, 2) * DT, DT), DT)]
            sem = tile_sem.at[lax.rem(u, 2)]
            if not start:
                copy(dst, dst, sem).wait()
                return
            down, _, b = place(u)

            @pl.when(down)
            def _():
                copy(gs.at[pl.ds(0, n_tok), cols(b, DT)], dst, sem).start()

            @pl.when(jnp.logical_not(down))
            def _():
                copy(qs.at[pl.ds(0, n_tok), cols(b, DT)], dst, sem).start()

        def part_slot(t):
            z = lax.rem(t, 3)
            return jnp.where(z == 2, 4, z + 1)

        def wait_part(t):
            q = part_slot(t)
            copy(dbuf.at[q], dbuf.at[q], part_sem.at[lax.rem(t, 3)]).wait()

        def unit(u, carry):
            down, hf, b = place(u)
            c0 = lax.rem(u, 2) * DT

            @pl.when((u == lo) | (b == 0))
            def _():
                @pl.when(down)
                def _():
                    copy(es.at[pl.ds(0, n_tok), cols(hf, CT)], ring.at[2], held_sem).start()

                @pl.when(jnp.logical_not(down))
                def _():
                    copy(hs.at[pl.ds(0, n_tok), cols(hf, CT)], ring.at[2], held_sem).start()

            @pl.when(u == lo)
            def _():
                tile(u, True)

            @pl.when(u + 1 < hi)
            def _():
                tile(u + 1, True)

            @pl.when((u == lo) | (b == 0))
            def _():
                copy(ring.at[2], ring.at[2], held_sem).wait()

            tile(u, False)
            def half_unit(z, carry):
                t = 2 * (u - lo) + z
                q = part_slot(t)

                @pl.when(t >= 3)
                def _():
                    wait_part(t)

                @pl.when(down)
                def _():
                    dbuf[q] = dot(ring[3, :, pl.ds(pl.multiple_of(c0 + z * ROWS, ROWS), ROWS)], ring[2], TN)
                    copy(dbuf.at[q], down_part.at[cols(2 * b + z, ROWS), cols(hf, CT)], part_sem.at[lax.rem(t, 3)]).start()

                @pl.when(jnp.logical_not(down))
                def _():
                    for a in range(2):
                        r = 2 * z + a
                        dbuf[q, :, pl.ds(a * DT, DT)] = dot(ring[2, :, cols(r, ROWS)], ring[3, :, pl.ds(pl.multiple_of(c0, DT), DT)], TN)
                    for a in range(2):
                        r = 2 * z + a
                        copy(dbuf.at[q, :, pl.ds(a * DT, DT)], up_part.at[cols(4 * hf + r, ROWS), cols(b, DT)], part_sem.at[lax.rem(t, 3)]).start()
                return carry

            lax.fori_loop(0, 2, half_unit, 0)
            return carry

        lax.fori_loop(lo, hi, unit, 0)

        @pl.when(hi > lo)
        def _():
            wait_part(2 * (hi - lo) - 1)
            wait_part(2 * (hi - lo) - 2)

        @pl.when(hi > lo + 1)
        def _():
            wait_part(2 * (hi - lo) - 3)

    barrier = pltpu.get_barrier_semaphore()

    def hello(**to):
        pl.semaphore_signal(barrier, inc=1, device_id=to, device_id_type=pl.DeviceIdType.MESH)

    @pl.when(jnp.logical_not(first))
    def _():
        hello(stage=s - 1)

    @pl.when(jnp.logical_not(last))
    def _():
        hello(stage=s + 1)

    @pl.when(last)
    def _():
        hello(data=peer)

    @pl.when(first)
    def _():
        load_in(0)

    start_f1(0)
    for j in range(NSTEP):
        copy(w1.at[0, :, pl.ds(j * CT, CT)], w1r.at[:, pl.ds(j * CT, CT)], w1_sem.at[j]).start()
        if j == 0:
            start_f1(1)
    for j in range(NSTEP):
        copy(w2.at[0, pl.ds(0, half), pl.ds(j * DT, DT)], w2r.at[:, pl.ds(j * DT, DT)], w2_sem.at[j]).start()
    loss_acc[...] = jnp.zeros_like(loss_acc)

    @pl.when(first)
    def _():
        pl.semaphore_wait(barrier, 1)

    @pl.when(jnp.logical_not(first))
    def _():
        pl.semaphore_wait(barrier, 2)

    def slot(k, carry):
        is_f, i = order(k)
        p = lax.rem(k, 2)

        @pl.when(k > 0)
        def _():
            copy(gq, gq, gq_sem).wait()

        @pl.when(jnp.logical_not(ahead(k)))
        def _():
            load_in(k)

        @pl.when(needs_copy(k))
        def _():
            copy(inb.at[p], inb.at[p], in_sem.at[p]).wait()

        @pl.when(is_f & first)
        def _():
            copy(inb.at[p], hs.at[rows(i)], st_sem).start()

        @pl.when(jnp.logical_not(is_f) & last)
        def _():
            copy(inb.at[p], es.at[rows(i)], st_sem).start()

        @pl.when(is_f & last)
        def _():
            copy(y.at[rows(i)], inb.at[1 - p], y_sem).start()

        @pl.when(is_f)
        def _():
            forward(k, i)

        @pl.when(jnp.logical_not(is_f))
        def _():
            backward(k, i)

        @pl.when((is_f & first) | (jnp.logical_not(is_f) & last))
        def _():
            copy(inb.at[p], inb.at[p], st_sem).wait()

        @pl.when(jnp.logical_not(is_f))
        def _():
            early(i)

        return carry

    lax.fori_loop(0, n_slot, slot, 0)
    copy(gq, gq, gq_sem).wait()
    for k in range(n_slot - 2, n_slot):
        wait_sent(jnp.int32(k))

    def to_peer():
        return pltpu.make_async_remote_copy(
            src_ref=lbuf.at[0], dst_ref=lbuf.at[1], send_sem=l_send.at[0], recv_sem=l_recv.at[0],
            device_id={'data': peer}, device_id_type=pl.DeviceIdType.MESH)

    def to_prev():
        return pltpu.make_async_remote_copy(
            src_ref=lbuf.at[2], dst_ref=lbuf.at[2], send_sem=l_send.at[1], recv_sem=l_recv.at[1],
            device_id={'stage': s - 1}, device_id_type=pl.DeviceIdType.MESH)

    @pl.when(last)
    def _():
        lbuf[0] = loss_acc[pl.ds(0, 8), :] + loss_acc[pl.ds(8, 8), :]
        rdma = to_peer()
        rdma.start()
        rdma.wait()
        lbuf[2] = lbuf[0] + lbuf[1]

    @pl.when(jnp.logical_not(last))
    def _():
        copy(lbuf.at[2], lbuf.at[2], l_recv.at[1]).wait()

    loss_out[...] = lbuf[2]

    @pl.when(jnp.logical_not(first))
    def _():
        to_prev().start()
        copy(lbuf.at[2], lbuf.at[2], l_send.at[1]).wait()


def run_pipeline(n_stage, n_data, x, y, w1, w2):
    n_row, width = x.shape
    ffn = w1.shape[2]
    n_chunk = n_row // ROWS
    half = ffn // 2
    hbm = pl.BlockSpec(memory_space=pl.ANY)
    out = jax.ShapeDtypeStruct
    dma = pltpu.SemaphoreType.DMA
    flops = 8 * n_row * width * ffn
    return pl.pallas_call(
        functools.partial(pipeline_kernel, n_stage, n_data, n_chunk, 1.0 / (n_data * n_row)),
        out_shape=(out((n_row, width), BF16), out((n_row, ffn), BF16), out((n_row, ffn), F32),
                   out((n_row, ffn), BF16), out((n_row, width), BF16), out((width, ffn), F32), out((ffn, width), F32), out((8, DT), F32)),
        in_specs=[hbm] * 4,
        out_specs=(hbm,) * 7 + (pl.BlockSpec(memory_space=pltpu.VMEM),),
        scratch_shapes=[
            pltpu.VMEM((width, half), BF16), pltpu.VMEM((half, width), BF16),
            pltpu.VMEM((RING, width, CT), BF16), pltpu.VMEM((ROWS, ffn), BF16),
            pltpu.VMEM((5, ROWS, CT), F32), pltpu.VMEM((2, ROWS, width), BF16),
            pltpu.VMEM((2, ROWS, width), BF16), pltpu.VMEM((16, DT), F32),
            pltpu.VMEM((3, 8, DT), F32),
            dma((NSTEP,)), dma((NSTEP,)), dma((RING,)), dma((5,)), dma, dma((2,)), dma((2,)),
            dma((n_chunk,)), dma((n_chunk,)), dma, dma, dma((2,)), dma((2,)), dma, dma((2,)), dma((3,)),
        ],
        compiler_params=pltpu.CompilerParams(collective_id=0, has_side_effects=True, vmem_limit_bytes=67043328),
        cost_estimate=pl.CostEstimate(flops=flops, bytes_accessed=1 << 30, transcendentals=n_row * ffn),
        name='pipeline',
    )(x, y, w1, w2)


def grad_kernel(up, sc, held, lo, hi, part, *rest):
    got, o = rest if len(rest) == 2 else (None, rest[0])
    n = hi.shape[0]

    def product(rows_, tile):
        return dot(held[rows_, :], tile[...], TN) if up else dot(tile[...], held[rows_, :], TN)

    def finish(v):
        o[...] = v if got is None else v + got[...]

    @pl.when(pl.program_id(0) < sc[1])
    def _():
        finish(product(pl.ds(n, n), hi) + part[...])

    @pl.when(pl.program_id(0) >= sc[1])
    def _():
        finish(product(pl.ds(0, n), lo) + product(pl.ds(n, n), hi))


def weight_grad(up, held, streamed, part, side, n_done, got=None):
    n_row, width = held.shape
    half = width // 2
    n_tok = n_row // 2
    ffn = streamed.shape[1]
    shape = (half, DT) if up else (DT, half)

    def at(i, j):
        return (j, i) if up else (i, j)

    specs = [
        pl.BlockSpec((n_row, half), lambda b, sc: (0, sc[0])),
        pl.BlockSpec((n_tok, DT), lambda b, sc: (0, jnp.maximum(b, jnp.minimum(sc[1], N_BLOCK - 1)))),
        pl.BlockSpec((n_tok, DT), lambda b, sc: (1, b)),
        pl.BlockSpec(shape, lambda b, sc: at(jnp.minimum(b, jnp.maximum(sc[1] - 1, 0)), sc[0])),
    ]
    args = [held, streamed, streamed, part]
    if got is not None:
        specs.append(pl.BlockSpec(shape, lambda b, sc: at(b, 0)))
        args.append(got)
    return pl.pallas_call(
        functools.partial(grad_kernel, up),
        out_shape=jax.ShapeDtypeStruct((half, ffn) if up else (ffn, half), F32),
        grid_spec=pltpu.PrefetchScalarGridSpec(
            num_scalar_prefetch=1, grid=(ffn // DT,), in_specs=specs,
            out_specs=pl.BlockSpec(shape, lambda b, sc: at(b, 0))),
        compiler_params=pltpu.CompilerParams(dimension_semantics=('arbitrary',), vmem_limit_bytes=60 * 2**20),
        cost_estimate=pl.CostEstimate(flops=2 * n_row * half * ffn, bytes_accessed=2 * n_row * ffn + 8 * half * ffn, transcendentals=0),
        name='grad_up' if up else 'grad_down',
    )(jnp.stack([side, n_done]).astype(jnp.int32), *args)


def solution(mesh):
    n_stage = mesh.shape['stage']
    n_data = mesh.shape['data']

    def per_device(inputs, targets, w_up, w_down):
        n_micro, n_tok, width = inputs.shape
        n_row = n_micro * n_tok
        x = inputs.reshape(n_row, width)
        y = targets.reshape(n_row, width)
        hs, gs, _, qs, es, up_part, down_part, loss = run_pipeline(n_stage, n_data, x, y, w_up, w_down)
        n_down, n_up, _, _ = early_plan(lax.axis_index('stage'))
        mine = lax.axis_index('data')
        other = n_data - 1 - mine
        swap = [(0, 1), (1, 0)]

        def grad(up, side, got=None):
            if up:
                return weight_grad(True, hs, qs, up_part, side, n_up, got)
            return weight_grad(False, es, gs, down_part, side, n_down, got)

        up_other = lax.ppermute(grad(True, other), 'data', swap)
        down_other = lax.ppermute(grad(False, other), 'data', swap)
        g_up = grad(True, mine, up_other)
        g_down = grad(False, mine, down_other)
        loss_total = jnp.sum(loss) * (0.5 / (n_data * n_row))
        return loss_total, g_up[None], g_down[None]

    return jax.shard_map(per_device, mesh=mesh, in_specs=(P('data', None, None), P('data', None, None), P('stage', None, None), P('stage', None, None)), out_specs=(P(), P('stage', 'data', None), P('stage', None, 'data')), check_vma=False)
```
